256 devices in a mesh: row: 32 (over z_hi, x, y), col: 8 (over z_lo, core).
Axes of the slice: x: 4, y: 4, z: 8 (z_hi: 2, z_lo: 4; z = z_hi * 4 + z_lo), core: 2. Of those that a mesh axis runs over, the one named last changes fastest.
Arguments:
- query_proj: bfloat16 [768, 768, 128], P('row', 'col'), may hold values from -8 to 8
- key_proj: bfloat16 [768, 768, 128], P('row', 'col'), may hold values from -8 to 8
- value_proj: bfloat16 [768, 768, 128], P('row', 'col'), may hold values from -6 to 6
- pair_bias: bfloat16 [4, 768, 768], P(None, 'col', 'row'), may hold values from -9 to 9
- pair_mask: int32 [768, 768], P('row', 'col'), may hold values 0 or 1
- grad_out: bfloat16 [768, 768, 128], P('row', 'col'), may hold values from -18 to 18
Outputs:
- grad_query: bfloat16 [768, 768, 128], P('row', 'col')
- grad_key: bfloat16 [768, 768, 128], P('row', 'col')
- grad_value: bfloat16 [768, 768, 128], P('row', 'col')
- grad_bias: float32 [4, 768, 768], P(None, 'col', 'row')
The draws below stay inside these ranges and needn't reach their ends.
All inputs are finite; a program needn't handle non-finite values. No bound on the sum of `pair_mask` on one device may be relied on, other than what follows from the above.
Results may differ from the reference program's by a relative error of at most 0.0096.
Values may be sent and summed in bfloat16 or wider, within the bound.
A program may use at most 128 MiB of HBM per device.

```python
import math
import jax
import jax.numpy as jnp
from jax import lax

HEADS = 4
HEAD_DIM = 32
RESIDUES = 768
CHANNELS = 128


def field_draw(key):
    return jnp.clip(jax.random.normal(key, (RESIDUES, RESIDUES, CHANNELS), jnp.float32), -6.0, 6.0)


def draw_query_proj(key, part):
    values_drawn = field_draw(jax.random.fold_in(key, 1))
    return values_drawn.astype(jnp.bfloat16)


def draw_key_proj(key, part):
    values_drawn = field_draw(jax.random.fold_in(key, 2))
    return values_drawn.astype(jnp.bfloat16)


def place_ends(values, own_key, least, top_value):
    dims = values.shape
    index_at = [jax.random.randint(jax.random.fold_in(own_key, axis), (), 0, dims[axis]) for axis in range(len(dims))]
    values = values.at[tuple(index_at)].set(least)
    longest = dims.index(max(dims))
    index_at[longest] = (index_at[longest] + 1) % dims[longest]
    return values.at[tuple(index_at)].set(top_value)


def steps_of(own_key, extent, split, least, largest):
    loudness, own = 1.0, jax.random.fold_in(own_key, 6)
    for dim, shards_of in split:
        heights = jnp.exp(jax.random.uniform(jax.random.fold_in(own, dim), (shards_of,), jnp.float32, least / len(split), largest / len(split)))
        loudness = loudness * jnp.repeat(heights, extent[dim] // shards_of).reshape([-1 if axis == dim else 1 for axis in range(len(extent))])
    return loudness


def noise(key, shape, deviation, limit, cuts=(), held_as=jnp.bfloat16):
    level = steps_of(key, shape, cuts, -0.22, 0.18) if cuts else 1.0
    result = jax.random.normal(key, shape, jnp.float32) * deviation * level
    return jnp.minimum(jnp.maximum(result, -limit), limit).astype(held_as)


def setup_inputs(seed: int = 0) -> dict:
    seeds = jax.random.split(jax.random.key(seed), 7)
    query_proj = draw_query_proj(jax.random.fold_in(seeds[6], 71), 0)
    key_proj = draw_key_proj(jax.random.fold_in(seeds[6], 71), 0)
    value_proj = noise(seeds[2], (RESIDUES, RESIDUES, CHANNELS), 1.0, 6.0, ((0, 32), (1, 8)))
    pair_bias = noise(seeds[3], (HEADS, RESIDUES, RESIDUES), 1.5, 9.0, ((1, 8), (2, 32)))
    pair_mask = place_ends((jax.random.randint(seeds[4], (RESIDUES, RESIDUES), 0, 4) < 3).astype(jnp.int32), jax.random.fold_in(seeds[4], 1), 0, 1)
    grad_out = noise(seeds[5], (RESIDUES, RESIDUES, CHANNELS), 3.0, 18.0, ((0, 32), (1, 8)))
    return {"query_proj": query_proj, "key_proj": key_proj, "value_proj": value_proj, "pair_bias": pair_bias, "pair_mask": pair_mask, "grad_out": grad_out}


def block_grads(queries, keys_all, values_all, grads, mask_all, bias_full):
    block_rows, query_count, channel_count = queries.shape
    key_count = keys_all.shape[1]
    scale = 1.0 / math.sqrt(HEAD_DIM)
    query_heads = queries.astype(jnp.float32).reshape(block_rows, query_count, HEADS, HEAD_DIM)
    key_heads = keys_all.astype(jnp.float32).reshape(block_rows, key_count, HEADS, HEAD_DIM)
    value_heads = values_all.astype(jnp.float32).reshape(block_rows, key_count, HEADS, HEAD_DIM)
    grad_heads = grads.astype(jnp.float32).reshape(block_rows, query_count, HEADS, HEAD_DIM)
    masked = 1000000000.0 * (mask_all.astype(jnp.float32) - 1.0)
    scores = jnp.einsum('bjhd,bkhd->bhjk', query_heads, key_heads) * scale
    scores = scores + bias_full.astype(jnp.float32)[None] + masked[:, None, None, :]
    top_score = lax.optimization_barrier(jnp.max(scores, axis=-1, keepdims=True))
    weights = jnp.exp(scores - top_score)
    attn_probs = weights / lax.optimization_barrier(jnp.sum(weights, axis=-1, keepdims=True))
    attn_low = attn_probs.astype(jnp.bfloat16).astype(jnp.float32)
    attended = jnp.einsum('bhjk,bkhd->bjhd', attn_low, value_heads)
    row_delta = lax.optimization_barrier(jnp.sum(grad_heads * attended, axis=-1))
    grad_probs = jnp.einsum('bjhd,bkhd->bhjk', grad_heads, value_heads)
    grad_scores = attn_probs * (grad_probs - jnp.transpose(row_delta, (0, 2, 1))[..., None])
    scores_low = grad_scores.astype(jnp.bfloat16).astype(jnp.float32)
    grad_queries = jnp.einsum('bhjk,bkhd->bjhd', scores_low, key_heads) * scale
    grad_keys = jnp.einsum('bhjk,bjhd->bkhd', scores_low, query_heads) * scale
    grad_values = jnp.einsum('bhjk,bjhd->bkhd', attn_low, grad_heads)
    bias_grad = lax.optimization_barrier(jnp.sum(grad_scores, axis=0))
    return (grad_queries.reshape(block_rows, query_count, channel_count), grad_keys.reshape(block_rows, key_count, channel_count), grad_values.reshape(block_rows, key_count, channel_count), bias_grad)

def reference(query_proj, key_proj, value_proj, pair_bias, pair_mask, grad_out):
    block_rows = math.gcd(RESIDUES, 8)
    steps_count = RESIDUES // block_rows

    def split_rows(array):
        return array.reshape((steps_count, block_rows) + array.shape[1:])

    def one_block(bias_sum, pieces):
        grad_queries, grad_keys, grad_values, bias_grad = block_grads(pieces[0], pieces[1], pieces[2], pieces[3], pieces[4], pair_bias)
        return (bias_sum + bias_grad, (grad_queries.astype(jnp.bfloat16), grad_keys.astype(jnp.bfloat16), grad_values.astype(jnp.bfloat16)))
    start_sum = jnp.zeros((HEADS, RESIDUES, RESIDUES), jnp.float32)
    bias_sum, stacked = lax.scan(one_block, start_sum, (split_rows(query_proj), split_rows(key_proj), split_rows(value_proj), split_rows(grad_out), split_rows(pair_mask)))
    full_shape = (RESIDUES, RESIDUES, CHANNELS)
    return (stacked[0].reshape(full_shape), stacked[1].reshape(full_shape), stacked[2].reshape(full_shape), bias_sum)
```

```python
import functools
import math

import jax
import jax.numpy as jnp
from jax import lax
from jax.experimental import pallas as pl
from jax.experimental.pallas import tpu as pltpu
from jax.sharding import Mesh
from jax.sharding import PartitionSpec as P

HEADS = 4
HEAD_DIM = 32
SCALE = 1.0 / math.sqrt(HEAD_DIM)
ROW = ("zh", "x", "y")
COL = ("zl", "core")
MESH = pl.DeviceIdType.MESH
LANES = 128
CHUNK = 256
F32 = jnp.float32
BF16 = jnp.bfloat16


def dot(a, b, dims):
    return lax.dot_general(a, b, (dims, ((), ())), preferred_element_type=F32)


def kernel(
    zs,
    cs,
    send_ref,
    mask_ref,
    bias_ref,
    out_ref,
    gb_ref,
    ab,
    biasf,
    mrecv,
    maskt,
    maskf,
    kq,
    vg,
    kt,
    vk,
    dqt,
    obuf,
    mask_ssem,
    mask_rsem,
    in_ssem,
    in_rsem,
    in_lsem,
    out_ssem,
    out_rsem,
    out_lsem,
):
    n = ab.shape[2]
    width = send_ref.shape[3]
    rows = ab.shape[0]
    groups = rows // 2
    peers = zs * cs
    tiles, _, tile, _ = bias_ref.shape
    zl, core = lax.axis_index("zl"), lax.axis_index("core")
    me = zl * cs + core

    def peer_of(offset):
        other = lax.rem(me + offset, peers)
        return other, other // cs, lax.rem(other, cs)

    def target(z, c):
        return {"zl": z, "core": c}

    barrier = pltpu.get_barrier_semaphore()
    for offset in range(1, peers):
        _, z, c = peer_of(offset)
        pl.semaphore_signal(barrier, inc=1, device_id=target(z, c), device_id_type=MESH)
    pl.semaphore_wait(barrier, peers - 1)

    my_columns = pl.ds(pl.multiple_of(me * width, width), width)

    def mask_copy(offset):
        _, z, c = peer_of(offset)
        return pltpu.make_async_remote_copy(
            src_ref=mask_ref.at[z],
            dst_ref=mrecv.at[me],
            send_sem=mask_ssem.at[offset],
            recv_sem=mask_rsem.at[offset],
            device_id=target(z, c),
            device_id_type=MESH,
        )

    def in_copy(group, offset):
        _, z, c = peer_of(offset)
        return pltpu.make_async_remote_copy(
            src_ref=send_ref.at[c, pl.ds(z * rows + group * 2, 2)],
            dst_ref=ab.at[pl.ds(group * 2, 2), :, my_columns],
            send_sem=in_ssem.at[group, offset],
            recv_sem=in_rsem.at[group, offset],
            device_id=target(z, c),
            device_id_type=MESH,
        )

    def in_local(group):
        return pltpu.make_async_copy(
            send_ref.at[core, pl.ds(zl * rows + group * 2, 2)],
            ab.at[pl.ds(group * 2, 2), :, my_columns],
            in_lsem.at[group],
        )

    def out_copy(group, offset):
        other, z, c = peer_of(offset)
        return pltpu.make_async_remote_copy(
            src_ref=obuf.at[group, :, pl.ds(pl.multiple_of(other * width, width), width)],
            dst_ref=out_ref.at[core, zl * groups + group],
            send_sem=out_ssem.at[group, offset],
            recv_sem=out_rsem.at[group, offset],
            device_id=target(z, c),
            device_id_type=MESH,
        )

    def out_local(group):
        return pltpu.make_async_copy(
            obuf.at[group, :, my_columns],
            out_ref.at[core, zl * groups + group],
            out_lsem.at[group],
        )

    for offset in range(1, peers):
        mask_copy(offset).start()
    mask_local = pltpu.make_async_copy(mask_ref.at[zl], mrecv.at[me], mask_ssem.at[0])
    mask_local.start()
    for group in range(groups):
        for offset in range(1, peers):
            in_copy(group, offset).start()
        in_local(group).start()

    def widen(r, carry):
        for h in range(2):
            biasf[h, pl.ds(pl.multiple_of(r * tile, 8), tile), :] = bias_ref[r, h].astype(F32)
        return carry

    lax.fori_loop(0, tiles, widen, 0)
    gb_ref[...] = jnp.zeros_like(gb_ref)

    mask_local.wait()
    for offset in range(1, peers):
        mask_copy(offset).wait()
    for s in range(peers):
        maskt[s * width : (s + 1) * width, :] = jnp.transpose(mrecv[s])[:width]
    for i in range(rows):
        maskf[i] = jnp.broadcast_to(maskt[:, i : i + 1], (n, LANES))

    lane_head = lax.broadcasted_iota(jnp.int32, (1, LANES), 1) // HEAD_DIM

    def one_group(group, carry):
        in_local(group).wait()
        for offset in range(1, peers):
            in_copy(group, offset).wait()

        def one_row(r, carry):
            i = group * 2 + r
            a = ab[i, 0].astype(F32)
            b = ab[i, 1].astype(F32)
            ar = pltpu.roll(a, 64, 1)
            br = pltpu.roll(b, 64, 1)
            for h in range(2):
                kq[h] = jnp.where(lane_head == h, ar, 0.0).astype(BF16)
                kq[2 + h] = jnp.where(lane_head == 2 + h, ar, 0.0).astype(BF16)
                vg[h] = jnp.where(lane_head == h, br, 0.0).astype(BF16)
                vg[2 + h] = jnp.where(lane_head == h, b, 0.0).astype(BF16)
            kt[...] = jnp.transpose(ar).astype(BF16)
            vk[...] = jnp.zeros_like(vk)

            def one_chunk(t, carry):
                h, ch = t // (n // CHUNK), lax.rem(t, n // CHUNK)
                cols = pl.ds(pl.multiple_of(ch * CHUNK, CHUNK), CHUNK)
                s = dot(kq[h], ab[i, 0, cols, :], ((1,), (1,)))
                dp = dot(vg[h], ab[i, 1, cols, :], ((1,), (1,)))
                m128 = maskf[i]
                mask = jnp.concatenate([m128] * (CHUNK // LANES), axis=1)
                s = (s * SCALE + biasf[h, :, cols]) + mask
                top = jnp.max(s, axis=0, keepdims=True)
                e = jnp.exp(s - top)
                inverse = 1.0 / jnp.sum(e, axis=0, keepdims=True)
                delta = jnp.sum(e * dp, axis=0, keepdims=True) * inverse
                p = e * inverse
                ds = p * (dp - delta)
                low = ds.astype(BF16)
                gb_ref[:, h, :, cols] += ds.reshape(tiles, tile, CHUNK)
                vk[...] += dot(p.astype(BF16), vg[2 + h, cols, :], ((1,), (0,))) + dot(
                    low, kq[2 + h, cols, :], ((1,), (0,))
                )
                head_rows = kt[pl.ds(pl.multiple_of(h * HEAD_DIM, HEAD_DIM), HEAD_DIM), :]
                at = pl.multiple_of(r * 64 + h * HEAD_DIM, HEAD_DIM)
                dqt[pl.ds(at, HEAD_DIM), cols] = dot(head_rows, low, ((1,), (0,)))
                return carry

            lax.fori_loop(0, 2 * (n // CHUNK), one_chunk, 0)
            obuf[group, r] = (vk[...] * jnp.where(lane_head < 2, 1.0, SCALE)).astype(BF16)
            return carry

        lax.fori_loop(0, 2, one_row, 0)
        obuf[group, 2] = (jnp.transpose(dqt[...]) * SCALE).astype(BF16)
        for offset in range(1, peers):
            out_copy(group, offset).start()
        out_local(group).start()
        return carry

    lax.fori_loop(0, groups, one_group, 0)

    def drain(group, carry):
        out_local(group).wait()
        for offset in range(1, peers):
            out_copy(group, offset).wait()
        return carry

    lax.fori_loop(0, groups, drain, 0)


def attention(zs, cs, send, mask, bias):
    width = send.shape[3]
    n = zs * cs * width
    rows = send.shape[1] // zs
    groups = rows // 2
    peers = zs * cs
    tiles, _, tile, _ = bias.shape
    any_spec = pl.BlockSpec(memory_space=pl.ANY)
    vmem_spec = pl.BlockSpec(memory_space=pltpu.VMEM)
    dma = pltpu.SemaphoreType.DMA
    return pl.pallas_call(
        functools.partial(kernel, zs, cs),
        out_shape=(
            jax.ShapeDtypeStruct((cs, zs * groups, 3, width, LANES), BF16),
            jax.ShapeDtypeStruct((tiles, 2, tile, n), F32),
        ),
        in_specs=[any_spec, any_spec, vmem_spec],
        out_specs=(any_spec, vmem_spec),
        scratch_shapes=[
            pltpu.VMEM((rows, 2, n, LANES), BF16),
            pltpu.VMEM((2, n, n), F32),
            pltpu.VMEM((peers, 8, LANES), F32),
            pltpu.VMEM((n, 8), F32),
            pltpu.VMEM((rows, n, LANES), F32),
            pltpu.VMEM((4, n, LANES), BF16),
            pltpu.VMEM((4, n, LANES), BF16),
            pltpu.VMEM((LANES, n), BF16),
            pltpu.VMEM((n, LANES), F32),
            pltpu.VMEM((LANES, n), F32),
            pltpu.VMEM((groups, 3, n, LANES), BF16),
            dma((peers,)),
            dma((peers,)),
            dma((groups, peers)),
            dma((groups, peers)),
            dma((groups,)),
            dma((groups, peers)),
            dma((groups, peers)),
            dma((groups,)),
        ],
        compiler_params=pltpu.CompilerParams(
            collective_id=0, has_side_effects=True, vmem_limit_bytes=56 * 1024 * 1024
        ),
        cost_estimate=pl.CostEstimate(
            flops=10 * rows * 2 * n * n * LANES, bytes_accessed=32 * 1024 * 1024, transcendentals=0
        ),
        name="attention_backward",
    )(send, mask, bias)


def local(zs, cs, query_proj, key_proj, value_proj, pair_bias, pair_mask, grad_out):
    rows, width, _ = query_proj.shape
    core = lax.axis_index("core")
    half = HEADS // 2 * HEAD_DIM

    bias = jnp.transpose(pair_bias, (0, 2, 1))
    bias = lax.all_gather(bias, COL, axis=2, tiled=True)
    bias = lax.dynamic_slice_in_dim(bias, core * 2, 2, 0)
    bias = lax.all_gather(bias, ROW, axis=0, tiled=False)

    def pack(a, b):
        return jnp.stack(
            [jnp.concatenate([a[..., c * half : (c + 1) * half], b[..., c * half : (c + 1) * half]], -1) for c in range(cs)]
        )

    send = jnp.stack([pack(query_proj, key_proj), pack(grad_out, value_proj)], 2)
    mask = 1000000000.0 * (pair_mask.astype(F32) - 1.0)
    per_chip = rows // zs
    mask = jnp.pad(mask.reshape(zs, per_chip, width), ((0, 0), (0, 8 - per_chip), (0, LANES - width)))

    out, gb = attention(zs, cs, send, mask, bias)

    gb = lax.psum_scatter(gb, ROW, scatter_dimension=0, tiled=False)
    tile = gb.shape[1]
    gb = gb.reshape(2, tile, zs * cs, width).transpose(2, 0, 1, 3)
    gb = lax.all_to_all(gb, COL, split_axis=0, concat_axis=0, tiled=True)
    gb = gb.reshape(zs, cs, 2, tile, width).sum(axis=0).reshape(HEADS, tile, width)
    grad_bias = jnp.transpose(gb, (0, 2, 1))

    def rejoin(pieces):
        return jnp.concatenate([pieces[c] for c in range(cs)], axis=-1)

    value_key = out[:, :, :2].reshape(cs, rows, width, LANES)
    grad_value = rejoin(value_key[..., :half])
    grad_key = rejoin(value_key[..., half:])
    pairs = out[:, :, 2]
    pairs = jnp.stack([pairs[..., :half], pairs[..., half:]], axis=2).reshape(cs, rows, width, half)
    grad_query = rejoin(pairs)
    return grad_query, grad_key, grad_value, grad_bias


def solution(mesh):
    rows = mesh.shape["row"]
    shape = (2, 4, 4, 4, 2) if rows == 32 else (1, 1, rows, 4, 2)
    torus = Mesh(mesh.devices.reshape(shape), ROW + COL)
    pair = P(ROW, COL, None)
    tile = P(None, COL, ROW)
    return jax.shard_map(
        functools.partial(local, 4, 2),
        mesh=torus,
        in_specs=(pair, pair, pair, tile, P(ROW, COL), pair),
        out_specs=(pair, pair, pair, tile),
        check_vma=False,
    )
```

```python
import functools
import math

import jax
import jax.numpy as jnp
from jax import lax
from jax.experimental import pallas as pl
from jax.experimental.pallas import tpu as pltpu
from jax.sharding import Mesh
from jax.sharding import PartitionSpec as P

HEADS = 4
HEAD_DIM = 32
SCALE = 1.0 / math.sqrt(HEAD_DIM)
ROW = ("zh", "x", "y")
COL = ("zl", "core")
MESH = pl.DeviceIdType.MESH
LANES = 128
CHUNK = 256
F32 = jnp.float32
BF16 = jnp.bfloat16


def dot(a, b, dims):
    return lax.dot_general(a, b, (dims, ((), ())), preferred_element_type=F32)


def kernel(
    dims,
    send_ref,
    mask_ref,
    tile_ref,
    out_ref,
    gout_ref,
    ab,
    biasb,
    biasf,
    gb,
    mrecv,
    maskt,
    maskf,
    kq,
    vg,
    kt,
    vk,
    dqt,
    obuf,
    trecv,
    first_s,
    first_r,
    second_s,
    second_r,
    partial,
    third_s,
    third_r,
    fourth_s,
    fourth_r,
    last_s,
    last_r,
    mask_sem,
    in_sem,
    in_lsem,
    out_sem,
    out_lsem,
    tile_sem,
    gather_sem,
    sum_sem,
    last_sem,
):
    zhs, zls, cs = dims
    n = ab.shape[2]
    width = send_ref.shape[3]
    tile = tile_ref.shape[2]
    rows = ab.shape[0]
    groups = rows // 2
    peers = zls * cs
    ring = zhs * peers
    chunk = min(CHUNK, n)
    chunks = n // chunk
    zh, zl, core = lax.axis_index("zh"), lax.axis_index("zl"), lax.axis_index("core")
    place = {"x": lax.axis_index("x"), "y": lax.axis_index("y")}
    me = zl * cs + core
    spot = zh * peers + me

    def remote(src, dst, sem, device):
        return pltpu.make_async_remote_copy(
            src_ref=src,
            dst_ref=dst,
            send_sem=sem.at[0],
            recv_sem=sem.at[1],
            device_id=device,
            device_id_type=MESH,
        )

    def peer_of(offset):
        other = lax.rem(me + offset, peers)
        return other, other // cs, lax.rem(other, cs)

    def ring_of(offset):
        other = lax.rem(spot + offset, ring)
        return other // peers, lax.rem(other, peers) // cs, lax.rem(other, cs)

    def ring_target(offset):
        h, z, c = ring_of(offset)
        return {"zh": h, "zl": z, "core": c}

    def step(axis, by):
        return lax.rem(place[axis] + by, 4)

    barrier = pltpu.get_barrier_semaphore()
    for offset in range(1, ring):
        pl.semaphore_signal(barrier, inc=1, device_id=ring_target(offset), device_id_type=MESH)
    for axis in ("x", "y"):
        for by in (1, 3):
            pl.semaphore_signal(barrier, inc=1, device_id={axis: step(axis, by)}, device_id_type=MESH)
    pl.semaphore_wait(barrier, ring - 1 + 4)

    def columns_of(c):
        return pl.ds(pl.multiple_of(c * width, width), width)

    def tile_copy(offset):
        _, _, c = ring_of(offset)
        return remote(tile_ref.at[c], trecv.at[spot], tile_sem.at[offset], ring_target(offset))

    def mask_copy(offset):
        _, z, c = peer_of(offset)
        return remote(mask_ref.at[z], mrecv.at[me], mask_sem.at[offset], {"zl": z, "core": c})

    def in_copy(group, offset):
        _, z, c = peer_of(offset)
        return remote(
            send_ref.at[c, pl.ds(z * rows + group * 2, 2)],
            ab.at[pl.ds(group * 2, 2), :, columns_of(me)],
            in_sem.at[group, offset],
            {"zl": z, "core": c},
        )

    def in_local(group):
        return pltpu.make_async_copy(
            send_ref.at[core, pl.ds(zl * rows + group * 2, 2)],
            ab.at[pl.ds(group * 2, 2), :, columns_of(me)],
            in_lsem.at[group],
        )

    def out_copy(group, offset):
        other, z, c = peer_of(offset)
        return remote(
            obuf.at[group, :, columns_of(other)],
            out_ref.at[core, zl * groups + group],
            out_sem.at[group, offset],
            {"zl": z, "core": c},
        )

    def out_local(group):
        return pltpu.make_async_copy(
            obuf.at[group, :, columns_of(me)],
            out_ref.at[core, zl * groups + group],
            out_lsem.at[group],
        )

    orders = (("x", "y"), ("y", "x"))

    def block(h, phase, index, half):
        axis = orders[h][phase]
        other = "y" if axis == "x" else "x"
        at = {axis: index, other: place[other] if phase == 0 else slice(None)}
        return biasb.at[h, slice(None) if half is None else half, at["x"], at["y"]]

    def gather_copy(h, phase, hop, way):
        axis = orders[h][phase]
        by = (1, 3)[way]
        if hop == 0:
            ref = block(h, phase, place[axis], None)
        else:
            ref = block(h, phase, step(axis, 4 - by), way)
        return remote(ref, ref, gather_sem.at[h, phase, hop, way], {axis: step(axis, by)})

    tile_local = pltpu.make_async_copy(tile_ref.at[core], trecv.at[spot], tile_sem.at[0, 0])
    mask_local = pltpu.make_async_copy(mask_ref.at[zl], mrecv.at[me], mask_sem.at[0, 0])
    for offset in range(1, ring):
        tile_copy(offset).start()
    tile_local.start()
    for offset in range(1, peers):
        mask_copy(offset).start()
    mask_local.start()
    for group in range(groups):
        for offset in range(1, peers):
            in_copy(group, offset).start()
        in_local(group).start()

    gb[...] = jnp.zeros_like(gb)

    tile_local.wait()
    for offset in range(1, ring):
        tile_copy(offset).wait()
    for h in range(2):
        for z in range(zhs):
            pieces = [trecv[z * peers + c, h].astype(F32)[:, :width] for c in range(peers)]
            biasb[h, z, place["x"], place["y"]] = jnp.concatenate(pieces, axis=1).astype(BF16)
    for phase in range(2):
        for h in range(2):
            for way in range(2):
                gather_copy(h, phase, 0, way).start()
        for h in range(2):
            for way in range(2):
                gather_copy(h, phase, 0, way).wait_recv()
                gather_copy(h, phase, 1, way).start()
        if phase == 0:
            mask_local.wait()
            for offset in range(1, peers):
                mask_copy(offset).wait()
            for s in range(peers):
                maskt[s * width : (s + 1) * width, :] = jnp.transpose(mrecv[s])[:width]
            for i in range(rows):
                maskf[i] = jnp.broadcast_to(maskt[:, i : i + 1], (n, LANES))
        for h in range(2):
            for way in range(2):
                gather_copy(h, phase, 0, way).wait_send()
                gather_copy(h, phase, 1, way).wait()

    def widen(r, carry):
        for h in range(2):
            biasf[h, pl.ds(pl.multiple_of(r * tile, tile), tile), :] = biasb[
                h, r // 16, lax.rem(r // 4, 4), lax.rem(r, 4)
            ].astype(F32)
        return carry

    lax.fori_loop(0, n // tile, widen, 0)

    lane_head = lax.broadcasted_iota(jnp.int32, (1, LANES), 1) // HEAD_DIM

    def terms(h, a, zsel):
        axis = orders[h][0]
        return gb[h, zsel, a] if axis == "x" else gb[h, zsel, :, a]

    def first_copy(h, way):
        axis = orders[h][0]
        return remote(
            first_s.at[h, way], first_r.at[h, way], sum_sem.at[h, 0, way], {axis: step(axis, (1, 3)[way])}
        )

    def second_copy(h, way, z):
        axis = orders[h][0]
        return remote(
            second_s.at[h, way, z],
            second_r.at[h, way, z],
            sum_sem.at[h, 1 + z, way],
            {axis: step(axis, (1, 3)[way])},
        )

    def third_copy(h, way):
        axis = orders[h][1]
        return remote(
            third_s.at[h, way], third_r.at[h, way], sum_sem.at[h, 3, way], {axis: step(axis, (1, 3)[way])}
        )

    def fourth_copy(h, way, z):
        axis = orders[h][1]
        return remote(
            fourth_s.at[h, way, z],
            fourth_r.at[h, way, z],
            sum_sem.at[h, 4 + z, way],
            {axis: step(axis, (1, 3)[way])},
        )

    def sums_begin(h):
        axis = orders[h][0]
        for way in range(2):
            first_s[h, way] = terms(h, step(axis, 2), way).astype(BF16)
            first_copy(h, way).start()
        for way in range(2):
            second_s[h, way, 1 - way] = terms(h, step(axis, (1, 3)[way]), 1 - way).astype(BF16)
            second_copy(h, way, 1 - way).start()

    def sums_forward(h):
        axis = orders[h][0]
        for way in range(2):
            first_copy(h, way).wait()
            own = terms(h, step(axis, (1, 3)[way]), way)
            second_s[h, way, way] = (own + first_r[h, way].astype(F32)).astype(BF16)
            second_copy(h, way, way).start()

    def sums_turn(h):
        mine = place[orders[h][0]]
        axis = orders[h][1]
        for z in range(2):
            for way in range(2):
                second_copy(h, way, z).wait()
            partial[h, z] = terms(h, mine, z) + second_r[h, 0, z].astype(F32) + second_r[h, 1, z].astype(F32)
        for way in range(2):
            third_s[h, way] = partial[h, way, step(axis, 2)].astype(BF16)
            third_copy(h, way).start()
        for way in range(2):
            fourth_s[h, way, 1 - way] = partial[h, 1 - way, step(axis, (1, 3)[way])].astype(BF16)
            fourth_copy(h, way, 1 - way).start()

    def sums_close(h):
        axis = orders[h][1]
        for way in range(2):
            third_copy(h, way).wait()
            own = partial[h, way, step(axis, (1, 3)[way])]
            fourth_s[h, way, way] = (own + third_r[h, way].astype(F32)).astype(BF16)
            fourth_copy(h, way, way).start()

    def sums_last(h):
        mine = place[orders[h][1]]
        for z in range(2):
            for way in range(2):
                fourth_copy(h, way, z).wait()
            total = partial[h, z, mine] + fourth_r[h, 0, z].astype(F32) + fourth_r[h, 1, z].astype(F32)
            for c in range(peers):
                piece = total[:, c * width : (c + 1) * width]
                pad = jnp.zeros((tile, LANES - width), F32)
                last_s[z * peers + c, h] = jnp.concatenate([piece, pad], axis=1).astype(BF16)

    def last_copy(offset):
        return remote(
            last_s.at[lax.rem(spot + offset, ring)], last_r.at[spot], last_sem.at[offset], ring_target(offset)
        )

    def one_group(group, carry):
        in_local(group).wait()
        for offset in range(1, peers):
            in_copy(group, offset).wait()

        def prepare(r, carry):
            i = group * 2 + r
            a = ab[i, 0].astype(F32)
            b = ab[i, 1].astype(F32)
            ar = pltpu.roll(a, 64, 1)
            br = pltpu.roll(b, 64, 1)
            for h in range(2):
                kq[r, h] = jnp.where(lane_head == h, ar, 0.0).astype(BF16)
                kq[r, 2 + h] = jnp.where(lane_head == 2 + h, ar, 0.0).astype(BF16)
                vg[r, h] = jnp.where(lane_head == h, br, 0.0).astype(BF16)
                vg[r, 2 + h] = jnp.where(lane_head == h, b, 0.0).astype(BF16)
            kt[r] = jnp.transpose(ar).astype(BF16)
            vk[r] = jnp.zeros_like(vk[r])
            return carry

        lax.fori_loop(0, 2, prepare, 0)

        def one_head(h, carry):
            def one_chunk(t, carry):
                r, ch = t // chunks, lax.rem(t, chunks)
                i = group * 2 + r
                cols = pl.ds(pl.multiple_of(ch * chunk, chunk), chunk)
                s = dot(kq[r, h], ab[i, 0, cols, :], ((1,), (1,)))
                dp = dot(vg[r, h], ab[i, 1, cols, :], ((1,), (1,)))
                m128 = maskf[i]
                mask = jnp.concatenate([m128] * (chunk // LANES), axis=1) if chunk > LANES else m128[:, :chunk]
                s = (s * SCALE + biasf[h, :, cols]) + mask
                top = jnp.max(s, axis=0, keepdims=True)
                e = jnp.exp(s - top)
                inverse = 1.0 / jnp.sum(e, axis=0, keepdims=True)
                delta = jnp.sum(e * dp, axis=0, keepdims=True) * inverse
                p = e * inverse
                ds = p * (dp - delta)
                low = ds.astype(BF16)
                gb[h, :, :, :, :, cols] += ds.reshape(2, 4, 4, tile, chunk)
                vk[r] += dot(p.astype(BF16), vg[r, 2 + h, cols, :], ((1,), (0,))) + dot(
                    low, kq[r, 2 + h, cols, :], ((1,), (0,))
                )
                head_rows = kt[r, pl.ds(pl.multiple_of(h * HEAD_DIM, HEAD_DIM), HEAD_DIM), :]
                at = pl.multiple_of(r * 64 + h * HEAD_DIM, HEAD_DIM)
                dqt[pl.ds(at, HEAD_DIM), cols] = dot(head_rows, low, ((1,), (0,)))
                return carry

            lax.fori_loop(0, 2 * chunks, one_chunk, 0)

            @pl.when((group == groups - 1) & (h == 0))
            def _():
                sums_begin(0)

            return carry

        lax.fori_loop(0, 2, one_head, 0)

        def finish(r, carry):
            obuf[group, r] = (vk[r] * jnp.where(lane_head < 2, 1.0, SCALE)).astype(BF16)
            return carry

        lax.fori_loop(0, 2, finish, 0)
        obuf[group, 2] = (jnp.transpose(dqt[...]) * SCALE).astype(BF16)
        for offset in range(1, peers):
            out_copy(group, offset).start()
        out_local(group).start()
        return carry

    lax.fori_loop(0, groups, one_group, 0)

    sums_begin(1)
    for stage in (sums_forward, sums_turn, sums_close, sums_last):
        for h in range(2):
            stage(h)
    for offset in range(1, ring):
        last_copy(offset).start()
    last_r[spot] = last_s[spot]

    def drain(group, carry):
        out_local(group).wait()
        for offset in range(1, peers):
            out_copy(group, offset).wait()
        return carry

    lax.fori_loop(0, groups, drain, 0)
    for offset in range(1, ring):
        last_copy(offset).wait()
    for c in range(cs):
        for h in range(2):
            total = last_r[c, h].astype(F32)
            for s in range(c + cs, ring, cs):
                total += last_r[s, h].astype(F32)
            gout_ref[2 * c + h] = total


def attention(dims, send, mask, tiles):
    zhs, zls, cs = dims
    width = send.shape[3]
    n = zls * cs * width
    rows = send.shape[1] // zls
    groups = rows // 2
    peers = zls * cs
    ring = zhs * peers
    tile = tiles.shape[2]
    any_spec = pl.BlockSpec(memory_space=pl.ANY)
    vmem_spec = pl.BlockSpec(memory_space=pltpu.VMEM)
    dma = pltpu.SemaphoreType.DMA
    return pl.pallas_call(
        functools.partial(kernel, dims),
        out_shape=(
            jax.ShapeDtypeStruct((cs, zls * groups, 3, width, LANES), BF16),
            jax.ShapeDtypeStruct((HEADS, tile, LANES), F32),
        ),
        in_specs=[any_spec, any_spec, any_spec],
        out_specs=(any_spec, vmem_spec),
        scratch_shapes=[
            pltpu.VMEM((rows, 2, n, LANES), BF16),
            pltpu.VMEM((2, 2, 4, 4, tile, n), BF16),
            pltpu.VMEM((2, n, n), F32),
            pltpu.VMEM((2, 2, 4, 4, tile, n), F32),
            pltpu.VMEM((peers, 8, LANES), F32),
            pltpu.VMEM((n, 8), F32),
            pltpu.VMEM((rows, n, LANES), F32),
            pltpu.VMEM((2, 4, n, LANES), BF16),
            pltpu.VMEM((2, 4, n, LANES), BF16),
            pltpu.VMEM((2, LANES, n), BF16),
            pltpu.VMEM((2, n, LANES), F32),
            pltpu.VMEM((LANES, n), F32),
            pltpu.VMEM((groups, 3, n, LANES), BF16),
            pltpu.VMEM((ring, 2, tile, LANES), BF16),
            pltpu.VMEM((2, 2, 4, tile, n), BF16),
            pltpu.VMEM((2, 2, 4, tile, n), BF16),
            pltpu.VMEM((2, 2, 2, 4, tile, n), BF16),
            pltpu.VMEM((2, 2, 2, 4, tile, n), BF16),
            pltpu.VMEM((2, 2, 4, tile, n), F32),
            pltpu.VMEM((2, 2, tile, n), BF16),
            pltpu.VMEM((2, 2, tile, n), BF16),
            pltpu.VMEM((2, 2, 2, tile, n), BF16),
            pltpu.VMEM((2, 2, 2, tile, n), BF16),
            pltpu.VMEM((ring, 2, tile, LANES), BF16),
            pltpu.VMEM((ring, 2, tile, LANES), BF16),
            dma((peers, 2)),
            dma((groups, peers, 2)),
            dma((groups,)),
            dma((groups, peers, 2)),
            dma((groups,)),
            dma((ring, 2)),
            dma((2, 2, 2, 2, 2)),
            dma((2, 6, 2, 2)),
            dma((ring, 2)),
        ],
        compiler_params=pltpu.CompilerParams(
            collective_id=0, has_side_effects=True, vmem_limit_bytes=60 * 1024 * 1024
        ),
        cost_estimate=pl.CostEstimate(
            flops=10 * rows * 2 * n * n * LANES, bytes_accessed=32 * 1024 * 1024, transcendentals=0
        ),
        name="attention_backward",
    )(send, mask, tiles)


def local(zhs, zs, cs, query_proj, key_proj, value_proj, pair_bias, pair_mask, grad_out):
    rows, width, _ = query_proj.shape
    half = HEADS // 2 * HEAD_DIM
    tile = pair_bias.shape[2]
    tiles = jnp.transpose(pair_bias, (0, 2, 1)).reshape(cs, 2, tile, width)
    tiles = jnp.pad(tiles, ((0, 0), (0, 0), (0, 0), (0, LANES - width)))

    def pack(a, b):
        return jnp.stack(
            [jnp.concatenate([a[..., c * half : (c + 1) * half], b[..., c * half : (c + 1) * half]], -1) for c in range(cs)]
        )

    send = jnp.stack([pack(query_proj, key_proj), pack(grad_out, value_proj)], 2)
    mask = 1000000000.0 * (pair_mask.astype(F32) - 1.0)
    per_chip = rows // zs
    mask = jnp.pad(mask.reshape(zs, per_chip, width), ((0, 0), (0, 8 - per_chip), (0, LANES - width)))

    out, gb = attention((zhs, zs, cs), send, mask, tiles)
    grad_bias = jnp.transpose(gb[:, :, :width], (0, 2, 1))

    def rejoin(pieces):
        return jnp.concatenate([pieces[c] for c in range(cs)], axis=-1)

    value_key = out[:, :, :2].reshape(cs, rows, width, LANES)
    grad_value = rejoin(value_key[..., :half])
    grad_key = rejoin(value_key[..., half:])
    pairs = out[:, :, 2]
    pairs = jnp.stack([pairs[..., :half], pairs[..., half:]], axis=2).reshape(cs, rows, width, half)
    grad_query = rejoin(pairs)
    return grad_query, grad_key, grad_value, grad_bias


def solution(mesh):
    shape = (2, 4, 4, mesh.shape["col"] // 2, 2)
    torus = Mesh(mesh.devices.reshape(shape), ROW + COL)
    pair = P(ROW, COL, None)
    tile = P(None, COL, ROW)
    return jax.shard_map(
        functools.partial(local, shape[0], shape[3], shape[4]),
        mesh=torus,
        in_specs=(pair, pair, pair, tile, P(ROW, COL), pair),
        out_specs=(pair, pair, pair, tile),
        check_vma=False,
    )
```

```python
import functools
import math

import jax
import jax.numpy as jnp
from jax import lax
from jax.experimental import pallas as pl
from jax.experimental.pallas import tpu as pltpu
from jax.sharding import Mesh
from jax.sharding import PartitionSpec as P

HEADS = 4
HEAD_DIM = 32
SCALE = 1.0 / math.sqrt(HEAD_DIM)
ROW = ("zh", "x", "y")
COL = ("zl", "core")
MESH = pl.DeviceIdType.MESH
LANES = 128
CHUNK = 256
F32 = jnp.float32
BF16 = jnp.bfloat16


def dot(a, b, dims):
    return lax.dot_general(a, b, (dims, ((), ())), preferred_element_type=F32)


def kernel(
    dims,
    q_ref,
    k_ref,
    v_ref,
    g_ref,
    mask_ref,
    tile_ref,
    dq_ref,
    dk_ref,
    dv_ref,
    gout_ref,
    send_ref,
    out_ref,
    pbuf,
    sbuf,
    dpbuf,
    lowbuf,
    maxbuf,
    ab,
    biasb,
    biasf,
    gb,
    mrecv,
    maskt,
    maskf,
    kq,
    vg,
    kt,
    vk,
    dqt,
    obuf,
    trecv,
    first_s,
    first_r,
    second_s,
    second_r,
    partial,
    third_s,
    third_r,
    fourth_s,
    fourth_r,
    last_s,
    last_r,
    mask_sem,
    in_sem,
    out_sem,
    tile_sem,
    gather_sem,
    sum_sem,
    last_sem,
):
    zhs, zls, cs = dims
    n = ab.shape[2]
    width = q_ref.shape[1]
    tile = tile_ref.shape[2]
    rows = ab.shape[0]
    groups = rows // 2
    peers = zls * cs
    ring = zhs * peers
    chunk = min(CHUNK, n)
    chunks = n // chunk
    span = n // 8
    zh, zl, core = lax.axis_index("zh"), lax.axis_index("zl"), lax.axis_index("core")
    place = {"x": lax.axis_index("x"), "y": lax.axis_index("y")}
    me = zl * cs + core
    spot = zh * peers + me

    def remote(src, dst, sem, device):
        return pltpu.make_async_remote_copy(
            src_ref=src,
            dst_ref=dst,
            send_sem=sem.at[0],
            recv_sem=sem.at[1],
            device_id=device,
            device_id_type=MESH,
        )

    def peer_of(offset):
        other = lax.rem(me + offset, peers)
        return other, other // cs, lax.rem(other, cs)

    def ring_of(offset):
        other = lax.rem(spot + offset, ring)
        return other // peers, lax.rem(other, peers) // cs, lax.rem(other, cs)

    def ring_target(offset):
        h, z, c = ring_of(offset)
        return {"zh": h, "zl": z, "core": c}

    def step(axis, by):
        return lax.rem(place[axis] + by, 4)

    low_half = lax.broadcasted_iota(jnp.int32, (1, 1, LANES), 2) < LANES // 2

    def join(a, b):
        a, b = a.astype(F32), b.astype(F32)
        shape = a.shape
        turn = lambda v: pltpu.roll(v.reshape(-1, LANES), LANES // 2, 1).reshape(shape)
        return jnp.where(low_half, a, turn(b)).astype(BF16), jnp.where(low_half, turn(a), b).astype(BF16)

    def pack(group):
        def pack_chip(z, carry):
            at = pl.ds(z * rows + group * 2, 2)
            first = join(q_ref[at], k_ref[at])
            second = join(g_ref[at], v_ref[at])
            for c in range(2):
                send_ref[c, at, 0] = first[c]
                send_ref[c, at, 1] = second[c]
            return carry

        lax.fori_loop(0, zls, pack_chip, 0)

    def unpack(group):
        def unpack_chip(z, carry):
            at = z * rows + group * 2
            pair = z * groups + group
            value, key = join(out_ref[0, pair, :2], out_ref[1, pair, :2])
            dv_ref[pl.ds(at, 2)] = value
            dk_ref[pl.ds(at, 2)] = key
            even, odd = join(out_ref[0, pair, 2:], out_ref[1, pair, 2:])
            dq_ref[pl.ds(at, 1)] = even
            dq_ref[pl.ds(at + 1, 1)] = odd
            return carry

        lax.fori_loop(0, zls, unpack_chip, 0)

    barrier = pltpu.get_barrier_semaphore()
    for offset in range(1, ring):
        pl.semaphore_signal(barrier, inc=1, device_id=ring_target(offset), device_id_type=MESH)
    for axis in ("x", "y"):
        for by in (1, 3):
            pl.semaphore_signal(barrier, inc=1, device_id={axis: step(axis, by)}, device_id_type=MESH)
    pl.semaphore_wait(barrier, ring - 1 + 4)

    def columns_of(c):
        return pl.ds(pl.multiple_of(c * width, width), width)

    def tile_copy(offset):
        _, _, c = ring_of(offset)
        return remote(tile_ref.at[c], trecv.at[spot], tile_sem.at[offset], ring_target(offset))

    def mask_copy(offset):
        _, z, c = peer_of(offset)
        return remote(mask_ref.at[z], mrecv.at[me], mask_sem.at[offset], {"zl": z, "core": c})

    def in_copy(group, offset):
        _, z, c = peer_of(offset)
        return remote(
            send_ref.at[c, pl.ds(z * rows + group * 2, 2)],
            ab.at[pl.ds(group * 2, 2), :, columns_of(me)],
            in_sem.at[group, offset],
            {"zl": z, "core": c},
        )

    def out_copy(group, offset):
        other, z, c = peer_of(offset)
        return remote(
            obuf.at[group, :, columns_of(other)],
            out_ref.at[core, zl * groups + group],
            out_sem.at[group, offset],
            {"zl": z, "core": c},
        )

    orders = (("x", "y"), ("y", "x"))

    def block(h, phase, index, half):
        axis = orders[h][phase]
        other = "y" if axis == "x" else "x"
        at = {axis: index, other: place[other] if phase == 0 else slice(None)}
        return biasb.at[h, slice(None) if half is None else half, at["x"], at["y"]]

    def gather_copy(h, phase, hop, way):
        axis = orders[h][phase]
        by = (1, 3)[way]
        if hop == 0:
            ref = block(h, phase, place[axis], None)
        else:
            ref = block(h, phase, step(axis, 4 - by), way)
        return remote(ref, ref, gather_sem.at[h, phase, hop, way], {axis: step(axis, by)})

    for offset in range(1, ring):
        tile_copy(offset).start()
    trecv[spot] = tile_ref[core]
    for offset in range(1, peers):
        mask_copy(offset).start()
    mrecv[me] = mask_ref[zl]
    for group in range(groups):
        pack(group)
        for offset in range(1, peers):
            in_copy(group, offset).start()
        ab[group * 2 : group * 2 + 2, :, columns_of(me)] = send_ref[core, pl.ds(zl * rows + group * 2, 2)]

    gb[...] = jnp.zeros_like(gb)

    for offset in range(1, ring):
        tile_copy(offset).wait()
    for h in range(2):
        for z in range(zhs):
            pieces = [trecv[z * peers + c, h].astype(F32) for c in range(peers)]
            biasb[h, z, place["x"], place["y"]] = jnp.concatenate(pieces, axis=1).astype(BF16)
    for phase in range(2):
        for h in range(2):
            for way in range(2):
                gather_copy(h, phase, 0, way).start()
        for h in range(2):
            for way in range(2):
                gather_copy(h, phase, 0, way).wait_recv()
                gather_copy(h, phase, 1, way).start()
        if phase == 0:
            for offset in range(1, peers):
                mask_copy(offset).wait()
            for s in range(peers):
                maskt[s * width : (s + 1) * width, :] = jnp.transpose(mrecv[s])
            for i in range(rows):
                maskf[i] = jnp.broadcast_to(maskt[:, i : i + 1], (n, LANES))
        for h in range(2):
            for way in range(2):
                gather_copy(h, phase, 0, way).wait_send()
                gather_copy(h, phase, 1, way).wait()

    def widen(r, carry):
        for h in range(2):
            biasf[h, pl.ds(pl.multiple_of(r * tile, tile), tile), :] = biasb[
                h, r // 16, lax.rem(r // 4, 4), lax.rem(r, 4)
            ].astype(F32)
        return carry

    lax.fori_loop(0, n // tile, widen, 0)

    lane_head = lax.broadcasted_iota(jnp.int32, (1, LANES), 1) // HEAD_DIM

    def terms(h, a, zsel):
        axis = orders[h][0]
        return gb[h, zsel, a] if axis == "x" else gb[h, zsel, :, a]

    def first_copy(h, way):
        axis = orders[h][0]
        return remote(
            first_s.at[h, way], first_r.at[h, way], sum_sem.at[h, 0, way], {axis: step(axis, (1, 3)[way])}
        )

    def second_copy(h, way, z):
        axis = orders[h][0]
        return remote(
            second_s.at[h, way, z],
            second_r.at[h, way, z],
            sum_sem.at[h, 1 + z, way],
            {axis: step(axis, (1, 3)[way])},
        )

    def third_copy(h, way):
        axis = orders[h][1]
        return remote(
            third_s.at[h, way], third_r.at[h, way], sum_sem.at[h, 3, way], {axis: step(axis, (1, 3)[way])}
        )

    def fourth_copy(h, way, z):
        axis = orders[h][1]
        return remote(
            fourth_s.at[h, way, z],
            fourth_r.at[h, way, z],
            sum_sem.at[h, 4 + z, way],
            {axis: step(axis, (1, 3)[way])},
        )

    def sums_begin(h):
        axis = orders[h][0]
        for way in range(2):
            first_s[h, way] = terms(h, step(axis, 2), way).astype(BF16)
            first_copy(h, way).start()
        for way in range(2):
            second_s[h, way, 1 - way] = terms(h, step(axis, (1, 3)[way]), 1 - way).astype(BF16)
            second_copy(h, way, 1 - way).start()

    def sums_forward(h):
        axis = orders[h][0]
        for way in range(2):
            first_copy(h, way).wait()
            own = terms(h, step(axis, (1, 3)[way]), way)
            second_s[h, way, way] = (own + first_r[h, way].astype(F32)).astype(BF16)
            second_copy(h, way, way).start()

    def sums_turn(h):
        mine = place[orders[h][0]]
        axis = orders[h][1]
        for z in range(2):
            for way in range(2):
                second_copy(h, way, z).wait()
            partial[h, z] = terms(h, mine, z) + second_r[h, 0, z].astype(F32) + second_r[h, 1, z].astype(F32)
        for way in range(2):
            third_s[h, way] = partial[h, way, step(axis, 2)].astype(BF16)
            third_copy(h, way).start()
        for way in range(2):
            fourth_s[h, way, 1 - way] = partial[h, 1 - way, step(axis, (1, 3)[way])].astype(BF16)
            fourth_copy(h, way, 1 - way).start()

    def sums_close(h):
        axis = orders[h][1]
        for way in range(2):
            third_copy(h, way).wait()
            own = partial[h, way, step(axis, (1, 3)[way])]
            fourth_s[h, way, way] = (own + third_r[h, way].astype(F32)).astype(BF16)
            fourth_copy(h, way, way).start()

    def sums_last(h):
        mine = place[orders[h][1]]
        for z in range(2):
            for way in range(2):
                fourth_copy(h, way, z).wait()
            total = partial[h, z, mine] + fourth_r[h, 0, z].astype(F32) + fourth_r[h, 1, z].astype(F32)
            for c in range(peers):
                last_s[z * peers + c, h] = total[:, c * width : (c + 1) * width].astype(BF16)

    def last_copy(offset):
        return remote(
            last_s.at[lax.rem(spot + offset, ring)], last_r.at[spot], last_sem.at[offset], ring_target(offset)
        )

    def one_group(group, carry):
        for offset in range(1, peers):
            in_copy(group, offset).wait()

        def prepare(r, carry):
            i = group * 2 + r
            a = ab[i, 0].astype(F32)
            b = ab[i, 1].astype(F32)
            ar = pltpu.roll(a, 64, 1)
            br = pltpu.roll(b, 64, 1)
            for h in range(2):
                kq[r, h] = jnp.where(lane_head == h, ar, 0.0).astype(BF16)
                kq[r, 2 + h] = jnp.where(lane_head == 2 + h, ar, 0.0).astype(BF16)
                vg[r, h] = jnp.where(lane_head == h, br, 0.0).astype(BF16)
                vg[r, 2 + h] = jnp.where(lane_head == h, b, 0.0).astype(BF16)
            kt[r] = jnp.transpose(ar).astype(BF16)
            vk[r] = jnp.zeros_like(vk[r])
            return carry

        lax.fori_loop(0, 2, prepare, 0)

        def where_of(u):
            h, ch = u // chunks, lax.rem(u, chunks)
            return h, pl.ds(pl.multiple_of(ch * chunk, chunk), chunk)

        def scores(r, u):
            h, cols = where_of(u)
            i = group * 2 + r
            s = dot(kq[r, h], ab[i, 0, cols, :], ((1,), (1,)))
            top = None
            for k0 in range(0, n, span):
                m128 = maskf[i, k0 : k0 + span, :]
                mask = jnp.concatenate([m128] * (chunk // LANES), axis=1) if chunk > LANES else m128[:, :chunk]
                part = (s[k0 : k0 + span] * SCALE + biasf[h, k0 : k0 + span, cols]) + mask
                sbuf[r, k0 : k0 + span] = part
                part = jnp.max(part.reshape(-1, 8, chunk), axis=0)
                top = part if top is None else jnp.maximum(top, part)
            maxbuf[r] = top
            dpbuf[r] = dot(vg[r, h], ab[i, 1, cols, :], ((1,), (1,)))

        def soft(r, u):
            h, cols = where_of(u)
            top = jnp.max(maxbuf[r], axis=0, keepdims=True)
            total = weighted = None
            for k0 in range(0, n, span):
                e = jnp.exp(sbuf[r, k0 : k0 + span] - top)
                sbuf[r, k0 : k0 + span] = e
                first = jnp.sum(e.reshape(-1, 8, chunk), axis=0)
                second = jnp.sum((e * dpbuf[r, k0 : k0 + span]).reshape(-1, 8, chunk), axis=0)
                total = first if total is None else total + first
                weighted = second if weighted is None else weighted + second
            inverse = 1.0 / jnp.sum(total, axis=0, keepdims=True)
            delta = jnp.sum(weighted, axis=0, keepdims=True) * inverse
            for b in range(8):
                k0 = b * span
                p = sbuf[r, k0 : k0 + span] * inverse
                ds = p * (dpbuf[r, k0 : k0 + span] - delta)
                pbuf[r, k0 : k0 + span] = p.astype(BF16)
                lowbuf[r, k0 : k0 + span] = ds.astype(BF16)
                gb[h, b // 4, b % 4, :, :, cols] += ds.reshape(4, tile, chunk)

        def grads(r, u):
            h, cols = where_of(u)
            vk[r] += dot(pbuf[r], vg[r, 2 + h, cols, :], ((1,), (0,))) + dot(
                lowbuf[r], kq[r, 2 + h, cols, :], ((1,), (0,))
            )
            head_rows = kt[r, pl.ds(pl.multiple_of(h * HEAD_DIM, HEAD_DIM), HEAD_DIM), :]
            at = pl.multiple_of(r * 64 + h * HEAD_DIM, HEAD_DIM)
            dqt[pl.ds(at, HEAD_DIM), cols] = dot(head_rows, lowbuf[r], ((1,), (0,)))

        steps = 2 * chunks
        pbuf[1] = jnp.zeros_like(pbuf[1])
        lowbuf[1] = jnp.zeros_like(lowbuf[1])
        scores(0, 0)

        def one_step(u, carry):
            scores(1, u)
            grads(1, lax.rem(u + steps - 1, steps))
            soft(0, u)
            scores(0, lax.rem(u + 1, steps))
            grads(0, u)
            soft(1, u)

            @pl.when((group == groups - 1) & (u == chunks - 1))
            def _():
                sums_begin(0)

            return carry

        lax.fori_loop(0, steps, one_step, 0)
        grads(1, steps - 1)

        def finish(r, carry):
            obuf[group, r] = (vk[r] * jnp.where(lane_head < 2, 1.0, SCALE)).astype(BF16)
            return carry

        lax.fori_loop(0, 2, finish, 0)
        obuf[group, 2] = (jnp.transpose(dqt[...]) * SCALE).astype(BF16)
        for offset in range(1, peers):
            out_copy(group, offset).start()
        out_ref[core, zl * groups + group] = obuf[group, :, columns_of(me)]
        return carry

    lax.fori_loop(0, groups, one_group, 0)

    sums_begin(1)
    for stage in (sums_forward, sums_turn, sums_close, sums_last):
        for h in range(2):
            stage(h)
    for offset in range(1, ring):
        last_copy(offset).start()
    last_r[spot] = last_s[spot]

    def drain(group, carry):
        for offset in range(1, peers):
            out_copy(group, offset).wait()
        unpack(group)
        return carry

    lax.fori_loop(0, groups, drain, 0)
    for offset in range(1, ring):
        last_copy(offset).wait()
    for c in range(cs):
        for h in range(2):
            total = last_r[c, h].astype(F32)
            for s in range(c + cs, ring, cs):
                total += last_r[s, h].astype(F32)
            gout_ref[2 * c + h] = total


def attention(dims, queries, keys, values, grads, mask, tiles):
    zhs, zls, cs = dims
    width = queries.shape[1]
    n = zls * cs * width
    rows = queries.shape[0] // zls
    chunk = min(CHUNK, n)
    groups = rows // 2
    peers = zls * cs
    ring = zhs * peers
    tile = tiles.shape[2]
    vmem_spec = pl.BlockSpec(memory_space=pltpu.VMEM)
    dma = pltpu.SemaphoreType.DMA
    return pl.pallas_call(
        functools.partial(kernel, dims),
        out_shape=(
            jax.ShapeDtypeStruct(queries.shape, BF16),
            jax.ShapeDtypeStruct(queries.shape, BF16),
            jax.ShapeDtypeStruct(queries.shape, BF16),
            jax.ShapeDtypeStruct((HEADS, tile, width), F32),
        ),
        in_specs=[vmem_spec] * 6,
        out_specs=(vmem_spec,) * 4,
        scratch_shapes=[
            pltpu.VMEM((cs, zls * rows, 2, width, LANES), BF16),
            pltpu.VMEM((cs, zls * groups, 3, width, LANES), BF16),
            pltpu.VMEM((2, n, chunk), BF16),
            pltpu.VMEM((2, n, chunk), F32),
            pltpu.VMEM((2, n, chunk), F32),
            pltpu.VMEM((2, n, chunk), BF16),
            pltpu.VMEM((2, 8, chunk), F32),
            pltpu.VMEM((rows, 2, n, LANES), BF16),
            pltpu.VMEM((2, 2, 4, 4, tile, n), BF16),
            pltpu.VMEM((2, n, n), F32),
            pltpu.VMEM((2, 2, 4, 4, tile, n), F32),
            pltpu.VMEM((peers, rows, width), F32),
            pltpu.VMEM((n, rows), F32),
            pltpu.VMEM((rows, n, LANES), F32),
            pltpu.VMEM((2, 4, n, LANES), BF16),
            pltpu.VMEM((2, 4, n, LANES), BF16),
            pltpu.VMEM((2, LANES, n), BF16),
            pltpu.VMEM((2, n, LANES), F32),
            pltpu.VMEM((LANES, n), F32),
            pltpu.VMEM((groups, 3, n, LANES), BF16),
            pltpu.VMEM((ring, 2, tile, width), BF16),
            pltpu.VMEM((2, 2, 4, tile, n), BF16),
            pltpu.VMEM((2, 2, 4, tile, n), BF16),
            pltpu.VMEM((2, 2, 2, 4, tile, n), BF16),
            pltpu.VMEM((2, 2, 2, 4, tile, n), BF16),
            pltpu.VMEM((2, 2, 4, tile, n), F32),
            pltpu.VMEM((2, 2, tile, n), BF16),
            pltpu.VMEM((2, 2, tile, n), BF16),
            pltpu.VMEM((2, 2, 2, tile, n), BF16),
            pltpu.VMEM((2, 2, 2, tile, n), BF16),
            pltpu.VMEM((ring, 2, tile, width), BF16),
            pltpu.VMEM((ring, 2, tile, width), BF16),
            dma((peers, 2)),
            dma((groups, peers, 2)),
            dma((groups, peers, 2)),
            dma((ring, 2)),
            dma((2, 2, 2, 2, 2)),
            dma((2, 6, 2, 2)),
            dma((ring, 2)),
        ],
        compiler_params=pltpu.CompilerParams(
            collective_id=0, has_side_effects=True, vmem_limit_bytes=63 * 1024 * 1024
        ),
        cost_estimate=pl.CostEstimate(
            flops=10 * rows * 2 * n * n * LANES, bytes_accessed=32 * 1024 * 1024, transcendentals=0
        ),
        name="attention_backward",
    )(queries, keys, values, grads, mask, tiles)


def local(zhs, zs, cs, query_proj, key_proj, value_proj, pair_bias, pair_mask, grad_out):
    rows, width, _ = query_proj.shape
    tile = pair_bias.shape[2]
    tiles = jnp.transpose(pair_bias, (0, 2, 1)).reshape(cs, 2, tile, width)
    mask = 1000000000.0 * (pair_mask.astype(F32) - 1.0)
    mask = mask.reshape(zs, rows // zs, width)
    grad_query, grad_key, grad_value, gb = attention(
        (zhs, zs, cs), query_proj, key_proj, value_proj, grad_out, mask, tiles
    )
    return grad_query, grad_key, grad_value, jnp.transpose(gb, (0, 2, 1))


def solution(mesh):
    shape = (2, 4, 4, mesh.shape["col"] // 2, 2)
    torus = Mesh(mesh.devices.reshape(shape), ROW + COL)
    pair = P(ROW, COL, None)
    tile = P(None, COL, ROW)
    return jax.shard_map(
        functools.partial(local, shape[0], shape[3], shape[4]),
        mesh=torus,
        in_specs=(pair, pair, pair, tile, P(ROW, COL), pair),
        out_specs=(pair, pair, pair, tile),
        check_vma=False,
    )
```

```python
import functools
import math

import jax
import jax.numpy as jnp
from jax import lax
from jax.experimental import pallas as pl
from jax.experimental.pallas import tpu as pltpu
from jax.sharding import Mesh
from jax.sharding import PartitionSpec as P

HEADS = 4
HEAD_DIM = 32
SCALE = 1.0 / math.sqrt(HEAD_DIM)
ROW = ("zh", "x", "y")
COL = ("zl", "core")
MESH = pl.DeviceIdType.MESH
LANES = 128
CHUNK = 256
F32 = jnp.float32
BF16 = jnp.bfloat16


def dot(a, b, dims):
    return lax.dot_general(a, b, (dims, ((), ())), preferred_element_type=F32)


def kernel(
    dims,
    q_hbm,
    k_hbm,
    v_hbm,
    g_hbm,
    mask_ref,
    tile_ref,
    dq_ref,
    dk_ref,
    dv_ref,
    gout_ref,
    loaded,
    send_ref,
    out_ref,
    pbuf,
    sbuf,
    dpbuf,
    lowbuf,
    maxbuf,
    ab,
    biasb,
    biasf,
    gb,
    mrecv,
    maskt,
    maskf,
    kq,
    vg,
    kt,
    vk,
    dqt,
    obuf,
    trecv,
    first_s,
    first_r,
    second_s,
    second_r,
    partial,
    third_s,
    third_r,
    fourth_s,
    fourth_r,
    last_s,
    last_r,
    load_sem,
    mask_sem,
    in_sem,
    out_sem,
    tile_sem,
    gather_sem,
    sum_sem,
    last_sem,
):
    zhs, zls, cs = dims
    n = ab.shape[2]
    width = loaded.shape[2]
    tile = tile_ref.shape[2]
    rows = ab.shape[0]
    groups = rows // 2
    peers = zls * cs
    ring = zhs * peers
    chunk = min(CHUNK, n)
    chunks = n // chunk
    span = n // 8
    zh, zl, core = lax.axis_index("zh"), lax.axis_index("zl"), lax.axis_index("core")
    place = {"x": lax.axis_index("x"), "y": lax.axis_index("y")}
    me = zl * cs + core
    spot = zh * peers + me

    def remote(src, dst, sem, device):
        return pltpu.make_async_remote_copy(
            src_ref=src,
            dst_ref=dst,
            send_sem=sem.at[0],
            recv_sem=sem.at[1],
            device_id=device,
            device_id_type=MESH,
        )

    def peer_of(offset):
        other = lax.rem(me + offset, peers)
        return other, other // cs, lax.rem(other, cs)

    def ring_of(offset):
        other = lax.rem(spot + offset, ring)
        return other // peers, lax.rem(other, peers) // cs, lax.rem(other, cs)

    def ring_target(offset):
        h, z, c = ring_of(offset)
        return {"zh": h, "zl": z, "core": c}

    def step(axis, by):
        return lax.rem(place[axis] + by, 4)

    low_half = lax.broadcasted_iota(jnp.int32, (1, 1, LANES), 2) < LANES // 2

    def join(a, b):
        a, b = a.astype(F32), b.astype(F32)
        shape = a.shape
        turn = lambda v: pltpu.roll(v.reshape(-1, LANES), LANES // 2, 1).reshape(shape)
        return jnp.where(low_half, a, turn(b)).astype(BF16), jnp.where(low_half, turn(a), b).astype(BF16)

    def pack(group):
        def pack_chip(z, carry):
            at = pl.ds(z * rows + group * 2, 2)
            first = join(loaded[0, at], loaded[1, at])
            second = join(loaded[3, at], loaded[2, at])
            for c in range(2):
                send_ref[c, at, 0] = first[c]
                send_ref[c, at, 1] = second[c]
            return carry

        lax.fori_loop(0, zls, pack_chip, 0)

    def unpack(group):
        def unpack_chip(z, carry):
            at = z * rows + group * 2
            pair = zls * rows + z * groups + group
            value, key = join(out_ref[0, pl.ds(at, 2)], out_ref[1, pl.ds(at, 2)])
            dv_ref[pl.ds(at, 2)] = value
            dk_ref[pl.ds(at, 2)] = key
            even, odd = join(out_ref[0, pl.ds(pair, 1)], out_ref[1, pl.ds(pair, 1)])
            dq_ref[pl.ds(at, 1)] = even
            dq_ref[pl.ds(at + 1, 1)] = odd
            return carry

        lax.fori_loop(0, zls, unpack_chip, 0)

    barrier = pltpu.get_barrier_semaphore()
    for offset in range(1, ring):
        pl.semaphore_signal(barrier, inc=1, device_id=ring_target(offset), device_id_type=MESH)
    for axis in ("x", "y"):
        for by in (1, 3):
            pl.semaphore_signal(barrier, inc=1, device_id={axis: step(axis, by)}, device_id_type=MESH)
    loads = [
        pltpu.make_async_copy(ref, loaded.at[i], load_sem.at[i])
        for i, ref in enumerate((q_hbm, k_hbm, v_hbm, g_hbm))
    ]
    for load in loads:
        load.start()
    for load in loads:
        load.wait()
    pack(0)
    pl.semaphore_wait(barrier, ring - 1 + 4)

    def columns_of(c):
        return pl.ds(pl.multiple_of(c * width, width), width)

    def tile_copy(offset):
        _, _, c = ring_of(offset)
        return remote(tile_ref.at[c], trecv.at[spot], tile_sem.at[offset], ring_target(offset))

    def mask_copy(offset):
        _, z, c = peer_of(offset)
        return remote(mask_ref.at[z], mrecv.at[me], mask_sem.at[offset], {"zl": z, "core": c})

    def in_copy(i, offset):
        _, z, c = peer_of(offset)
        return remote(
            send_ref.at[c, z * rows + i],
            ab.at[i, :, columns_of(me)],
            in_sem.at[i, offset],
            {"zl": z, "core": c},
        )

    def slot_of(i, pair):
        return (rows + i, zls * rows + zl * groups + i) if pair else (i, zl * rows + i)

    def out_copy(i, pair, offset):
        other, z, c = peer_of(offset)
        source, dest = slot_of(i, pair)
        return remote(
            obuf.at[source, columns_of(other)],
            out_ref.at[core, dest],
            out_sem.at[source, offset],
            {"zl": z, "core": c},
        )

    def out_start(i, pair):
        for offset in range(1, peers):
            out_copy(i, pair, offset).start()

    def out_keep(i, pair):
        source, dest = slot_of(i, pair)
        out_ref[core, dest] = obuf[source, columns_of(me)]

    orders = (("x", "y"), ("y", "x"))

    def block(h, phase, index, half):
        axis = orders[h][phase]
        other = "y" if axis == "x" else "x"
        at = {axis: index, other: place[other] if phase == 0 else slice(None)}
        return biasb.at[h, slice(None) if half is None else half, at["x"], at["y"]]

    def gather_copy(h, phase, hop, way):
        axis = orders[h][phase]
        by = (1, 3)[way]
        half = 1 - way if hop == 1 else way
        ref = block(h, phase, step(axis, 4 - by) if hop == 2 else place[axis], half)
        return remote(ref, ref, gather_sem.at[h, phase, hop, way], {axis: step(axis, by)})

    for offset in range(1, ring):
        tile_copy(offset).start()
    trecv[spot] = tile_ref[core]
    for offset in range(1, peers):
        mask_copy(offset).start()
    mrecv[me] = mask_ref[zl]
    for group in range(groups):
        if group:
            pack(group)
        for i in (group * 2, group * 2 + 1):
            for offset in range(1, peers):
                in_copy(i, offset).start()
        ab[group * 2 : group * 2 + 2, :, columns_of(me)] = send_ref[core, pl.ds(zl * rows + group * 2, 2)]

    gb[...] = jnp.zeros_like(gb)

    for offset in range(1, ring):
        tile_copy(offset).wait()
    for h in range(2):
        for z in range(zhs):
            pieces = [trecv[z * peers + c, h].astype(F32) for c in range(peers)]
            biasb[h, z, place["x"], place["y"]] = jnp.concatenate(pieces, axis=1).astype(BF16)
    for phase in range(2):
        for hop in range(2):
            for h in range(2):
                for way in range(2):
                    gather_copy(h, phase, hop, way).start()
        for h in range(2):
            for way in range(2):
                gather_copy(h, phase, 0, way).wait_recv()
                gather_copy(h, phase, 2, way).start()
        if phase == 0:
            for offset in range(1, peers):
                mask_copy(offset).wait()
            for s in range(peers):
                maskt[s * width : (s + 1) * width, :] = jnp.transpose(mrecv[s])
            for i in range(rows):
                maskf[i] = jnp.broadcast_to(maskt[:, i : i + 1], (n, LANES))
        for h in range(2):
            for way in range(2):
                gather_copy(h, phase, 0, way).wait_send()
                gather_copy(h, phase, 1, way).wait()
                gather_copy(h, phase, 2, way).wait()

    def widen(r, carry):
        for h in range(2):
            biasf[h, pl.ds(pl.multiple_of(r * tile, tile), tile), :] = biasb[
                h, r // 16, lax.rem(r // 4, 4), lax.rem(r, 4)
            ].astype(F32)
        return carry

    lax.fori_loop(0, n // tile, widen, 0)

    lane_head = lax.broadcasted_iota(jnp.int32, (1, LANES), 1) // HEAD_DIM

    def terms(h, a, zsel):
        axis = orders[h][0]
        return gb[h, zsel, a] if axis == "x" else gb[h, zsel, :, a]

    def first_copy(h, way):
        axis = orders[h][0]
        return remote(
            first_s.at[h, way], first_r.at[h, way], sum_sem.at[h, 0, way], {axis: step(axis, (1, 3)[way])}
        )

    def second_copy(h, way, z):
        axis = orders[h][0]
        return remote(
            second_s.at[h, way, z],
            second_r.at[h, way, z],
            sum_sem.at[h, 1 + z, way],
            {axis: step(axis, (1, 3)[way])},
        )

    def third_copy(h, way):
        axis = orders[h][1]
        return remote(
            third_s.at[h, way], third_r.at[h, way], sum_sem.at[h, 3, way], {axis: step(axis, (1, 3)[way])}
        )

    def fourth_copy(h, way, z):
        axis = orders[h][1]
        return remote(
            fourth_s.at[h, way, z],
            fourth_r.at[h, way, z],
            sum_sem.at[h, 4 + z, way],
            {axis: step(axis, (1, 3)[way])},
        )

    def sums_begin(h):
        axis = orders[h][0]
        for way in range(2):
            first_s[h, way] = terms(h, step(axis, 2), way).astype(BF16)
            first_copy(h, way).start()
        for way in range(2):
            second_s[h, way, 1 - way] = terms(h, step(axis, (1, 3)[way]), 1 - way).astype(BF16)
            second_copy(h, way, 1 - way).start()

    def sums_forward(h):
        axis = orders[h][0]
        for way in range(2):
            first_copy(h, way).wait()
            own = terms(h, step(axis, (1, 3)[way]), way)
            second_s[h, way, way] = (own + first_r[h, way].astype(F32)).astype(BF16)
            second_copy(h, way, way).start()

    def sums_turn(h):
        mine = place[orders[h][0]]
        axis = orders[h][1]
        for z in range(2):
            for way in range(2):
                second_copy(h, way, z).wait()
            partial[h, z] = terms(h, mine, z) + second_r[h, 0, z].astype(F32) + second_r[h, 1, z].astype(F32)
        for way in range(2):
            third_s[h, way] = partial[h, way, step(axis, 2)].astype(BF16)
            third_copy(h, way).start()
        for way in range(2):
            fourth_s[h, way, 1 - way] = partial[h, 1 - way, step(axis, (1, 3)[way])].astype(BF16)
            fourth_copy(h, way, 1 - way).start()

    def sums_close(h):
        axis = orders[h][1]
        for way in range(2):
            third_copy(h, way).wait()
            own = partial[h, way, step(axis, (1, 3)[way])]
            fourth_s[h, way, way] = (own + third_r[h, way].astype(F32)).astype(BF16)
            fourth_copy(h, way, way).start()

    def sums_last(h):
        mine = place[orders[h][1]]
        for z in range(2):
            for way in range(2):
                fourth_copy(h, way, z).wait()
            total = partial[h, z, mine] + fourth_r[h, 0, z].astype(F32) + fourth_r[h, 1, z].astype(F32)
            for c in range(peers):
                last_s[z * peers + c, h] = total[:, c * width : (c + 1) * width].astype(BF16)

    def last_copy(offset):
        return remote(
            last_s.at[lax.rem(spot + offset, ring)], last_r.at[spot], last_sem.at[offset], ring_target(offset)
        )

    def release(count):
        def release_row(i, carry):
            out_start(i, False)
            return carry

        def release_pair(i, carry):
            out_start(i, True)
            return carry

        lax.fori_loop(0, count, release_row, 0)
        lax.fori_loop(0, groups - 1, release_pair, 0)

    def one_row(i, last):
        for offset in range(1, peers):
            in_copy(i, offset).wait()
        if not last:
            pl.when(i == rows - 2)(lambda: release(rows - 2))
        a = ab[i, 0].astype(F32)
        b = ab[i, 1].astype(F32)
        ar = pltpu.roll(a, 64, 1)
        br = pltpu.roll(b, 64, 1)
        for h in range(2):
            kq[h] = jnp.where(lane_head == h, ar, 0.0).astype(BF16)
            kq[2 + h] = jnp.where(lane_head == 2 + h, ar, 0.0).astype(BF16)
            vg[h] = jnp.where(lane_head == h, br, 0.0).astype(BF16)
            vg[2 + h] = jnp.where(lane_head == h, b, 0.0).astype(BF16)
        kt[...] = jnp.transpose(ar).astype(BF16)
        vk[...] = jnp.zeros_like(vk)

        def columns(u):
            return pl.ds(pl.multiple_of(u * chunk, chunk), chunk)

        def scores(h, u):
            cols = columns(u)
            s = dot(kq[h], ab[i, 0, cols, :], ((1,), (1,)))
            top = None
            for k0 in range(0, n, span):
                m128 = maskf[i, k0 : k0 + span, :]
                mask = jnp.concatenate([m128] * (chunk // LANES), axis=1) if chunk > LANES else m128[:, :chunk]
                part = (s[k0 : k0 + span] * SCALE + biasf[h, k0 : k0 + span, cols]) + mask
                sbuf[h, k0 : k0 + span] = part
                part = jnp.max(part.reshape(-1, 8, chunk), axis=0)
                top = part if top is None else jnp.maximum(top, part)
            maxbuf[h] = top
            dpbuf[h] = dot(vg[h], ab[i, 1, cols, :], ((1,), (1,)))

        def soft(h, u):
            cols = columns(u)
            top = jnp.max(maxbuf[h], axis=0, keepdims=True)
            total = weighted = None
            for k0 in range(0, n, span):
                e = jnp.exp(sbuf[h, k0 : k0 + span] - top)
                sbuf[h, k0 : k0 + span] = e
                first = jnp.sum(e.reshape(-1, 8, chunk), axis=0)
                second = jnp.sum((e * dpbuf[h, k0 : k0 + span]).reshape(-1, 8, chunk), axis=0)
                total = first if total is None else total + first
                weighted = second if weighted is None else weighted + second
            inverse = 1.0 / jnp.sum(total, axis=0, keepdims=True)
            delta = jnp.sum(weighted, axis=0, keepdims=True) * inverse
            for b in range(8):
                k0 = b * span
                p = sbuf[h, k0 : k0 + span] * inverse
                ds = p * (dpbuf[h, k0 : k0 + span] - delta)
                pbuf[h, k0 : k0 + span] = p.astype(BF16)
                lowbuf[h, k0 : k0 + span] = ds.astype(BF16)
                gb[h, b // 4, b % 4, :, :, cols] += ds.reshape(4, tile, chunk)

        def grads(h, u):
            cols = columns(u)
            vk[...] += dot(pbuf[h], vg[2 + h, cols, :], ((1,), (0,))) + dot(
                lowbuf[h], kq[2 + h, cols, :], ((1,), (0,))
            )
            head_rows = kt[h * HEAD_DIM : (h + 1) * HEAD_DIM, :]
            at = pl.multiple_of(lax.rem(i, 2) * 64 + h * HEAD_DIM, HEAD_DIM)
            dqt[pl.ds(at, HEAD_DIM), cols] = dot(head_rows, lowbuf[h], ((1,), (0,)))

        pbuf[1] = jnp.zeros_like(pbuf[1])
        lowbuf[1] = jnp.zeros_like(lowbuf[1])
        scores(0, 0)

        def one_step(u, carry):
            scores(1, u)
            grads(1, lax.rem(u + chunks - 1, chunks))
            soft(0, u)
            scores(0, lax.rem(u + 1, chunks))
            grads(0, u)
            soft(1, u)
            return carry

        lax.fori_loop(0, chunks, one_step, 0)
        if last:
            sums_begin(0)
            sums_begin(1)
        grads(1, chunks - 1)
        obuf[i] = (vk[...] * jnp.where(lane_head < 2, 1.0, SCALE)).astype(BF16)
        if last:
            out_start(i, False)
        else:
            pl.when(i == rows - 2)(lambda: out_start(i, False))
        out_keep(i, False)

    def close_pair(pair):
        obuf[rows + pair] = (jnp.transpose(dqt[...]) * SCALE).astype(BF16)
        out_keep(pair, True)

    def early_row(i, carry):
        one_row(i, False)

        @pl.when(lax.rem(i, 2) == 1)
        def _():
            close_pair(i // 2)

        return carry

    lax.fori_loop(0, rows - 1, early_row, 0)
    one_row(rows - 1, True)
    sums_forward(0)
    sums_forward(1)
    close_pair(groups - 1)
    for stage in (sums_turn, sums_close, sums_last):
        for h in range(2):
            stage(h)
    for offset in range(1, ring):
        last_copy(offset).start()
    out_start(groups - 1, True)
    last_r[spot] = last_s[spot]

    def drain(group, carry):
        for offset in range(1, peers):
            out_copy(group * 2, False, offset).wait()
            out_copy(group * 2 + 1, False, offset).wait()
            out_copy(group, True, offset).wait()
        unpack(group)
        return carry

    lax.fori_loop(0, groups - 1, drain, 0)
    for offset in range(1, ring):
        last_copy(offset).wait()
    for c in range(cs):
        for h in range(2):
            total = last_r[c, h].astype(F32)
            for s in range(c + cs, ring, cs):
                total += last_r[s, h].astype(F32)
            gout_ref[2 * c + h] = total
    drain(groups - 1, 0)


def attention(dims, queries, keys, values, grads, mask, tiles):
    zhs, zls, cs = dims
    width = queries.shape[1]
    n = zls * cs * width
    rows = queries.shape[0] // zls
    chunk = min(CHUNK, n)
    groups = rows // 2
    peers = zls * cs
    ring = zhs * peers
    tile = tiles.shape[2]
    vmem_spec = pl.BlockSpec(memory_space=pltpu.VMEM)
    dma = pltpu.SemaphoreType.DMA
    return pl.pallas_call(
        functools.partial(kernel, dims),
        out_shape=(
            jax.ShapeDtypeStruct(queries.shape, BF16),
            jax.ShapeDtypeStruct(queries.shape, BF16),
            jax.ShapeDtypeStruct(queries.shape, BF16),
            jax.ShapeDtypeStruct((HEADS, tile, width), F32),
        ),
        in_specs=[pl.BlockSpec(memory_space=pl.ANY)] * 4 + [vmem_spec] * 2,
        out_specs=(vmem_spec,) * 4,
        scratch_shapes=[
            pltpu.VMEM((4, zls * rows, width, LANES), BF16),
            pltpu.VMEM((cs, zls * rows, 2, width, LANES), BF16),
            pltpu.VMEM((cs, zls * (rows + groups), width, LANES), BF16),
            pltpu.VMEM((2, n, chunk), BF16),
            pltpu.VMEM((2, n, chunk), F32),
            pltpu.VMEM((2, n, chunk), F32),
            pltpu.VMEM((2, n, chunk), BF16),
            pltpu.VMEM((2, 8, chunk), F32),
            pltpu.VMEM((rows, 2, n, LANES), BF16),
            pltpu.VMEM((2, 2, 4, 4, tile, n), BF16),
            pltpu.VMEM((2, n, n), F32),
            pltpu.VMEM((2, 2, 4, 4, tile, n), F32),
            pltpu.VMEM((peers, rows, width), F32),
            pltpu.VMEM((n, rows), F32),
            pltpu.VMEM((rows, n, LANES), F32),
            pltpu.VMEM((4, n, LANES), BF16),
            pltpu.VMEM((4, n, LANES), BF16),
            pltpu.VMEM((LANES, n), BF16),
            pltpu.VMEM((n, LANES), F32),
            pltpu.VMEM((LANES, n), F32),
            pltpu.VMEM((rows + groups, n, LANES), BF16),
            pltpu.VMEM((ring, 2, tile, width), BF16),
            pltpu.VMEM((2, 2, 4, tile, n), BF16),
            pltpu.VMEM((2, 2, 4, tile, n), BF16),
            pltpu.VMEM((2, 2, 2, 4, tile, n), BF16),
            pltpu.VMEM((2, 2, 2, 4, tile, n), BF16),
            pltpu.VMEM((2, 2, 4, tile, n), F32),
            pltpu.VMEM((2, 2, tile, n), BF16),
            pltpu.VMEM((2, 2, tile, n), BF16),
            pltpu.VMEM((2, 2, 2, tile, n), BF16),
            pltpu.VMEM((2, 2, 2, tile, n), BF16),
            pltpu.VMEM((ring, 2, tile, width), BF16),
            pltpu.VMEM((ring, 2, tile, width), BF16),
            dma((4,)),
            dma((peers, 2)),
            dma((rows, peers, 2)),
            dma((rows + groups, peers, 2)),
            dma((ring, 2)),
            dma((2, 2, 3, 2, 2)),
            dma((2, 6, 2, 2)),
            dma((ring, 2)),
        ],
        compiler_params=pltpu.CompilerParams(
            collective_id=0, has_side_effects=True, vmem_limit_bytes=52 * 1024 * 1024
        ),
        cost_estimate=pl.CostEstimate(
            flops=10 * rows * 2 * n * n * LANES, bytes_accessed=32 * 1024 * 1024, transcendentals=0
        ),
        name="attention_backward",
    )(queries, keys, values, grads, mask, tiles)


def local(zhs, zs, cs, query_proj, key_proj, value_proj, pair_bias, pair_mask, grad_out):
    rows, width, _ = query_proj.shape
    tile = pair_bias.shape[2]
    tiles = jnp.transpose(pair_bias, (0, 2, 1)).reshape(cs, 2, tile, width)
    mask = 1000000000.0 * (pair_mask.astype(F32) - 1.0)
    mask = mask.reshape(zs, rows // zs, width)
    grad_query, grad_key, grad_value, gb = attention(
        (zhs, zs, cs), query_proj, key_proj, value_proj, grad_out, mask, tiles
    )
    return grad_query, grad_key, grad_value, jnp.transpose(gb, (0, 2, 1))


def solution(mesh):
    shape = (2, 4, 4, mesh.shape["col"] // 2, 2)
    torus = Mesh(mesh.devices.reshape(shape), ROW + COL)
    pair = P(ROW, COL, None)
    tile = P(None, COL, ROW)
    return jax.shard_map(
        functools.partial(local, shape[0], shape[3], shape[4]),
        mesh=torus,
        in_specs=(pair, pair, pair, tile, P(ROW, COL), pair),
        out_specs=(pair, pair, pair, tile),
        check_vma=False,
    )
```

```python
import functools
import math

import jax
import jax.numpy as jnp
from jax import lax
from jax.experimental import pallas as pl
from jax.experimental.pallas import tpu as pltpu
from jax.sharding import Mesh
from jax.sharding import PartitionSpec as P

HEADS = 4
HEAD_DIM = 32
SCALE = 1.0 / math.sqrt(HEAD_DIM)
ROW = ("zh", "x", "y")
COL = ("zl", "core")
MESH = pl.DeviceIdType.MESH
LANES = 128
CHUNK = 256
F32 = jnp.float32
BF16 = jnp.bfloat16


def dot(a, b, dims):
    return lax.dot_general(a, b, (dims, ((), ())), preferred_element_type=F32)


def kernel(
    dims,
    q_hbm,
    k_hbm,
    v_hbm,
    g_hbm,
    mask_in,
    tile_ref,
    dq_ref,
    dk_ref,
    dv_ref,
    gout_ref,
    loaded,
    mask_ref,
    send_ref,
    out_ref,
    pbuf,
    sbuf,
    dpbuf,
    lowbuf,
    maxbuf,
    ab,
    biasb,
    biasf,
    gb,
    mrecv,
    maskt,
    maskf,
    kq,
    vg,
    kt,
    vk,
    dqt,
    obuf,
    trecv,
    first_s,
    first_r,
    second_s,
    second_r,
    partial,
    third_s,
    third_r,
    fourth_s,
    fourth_r,
    last_s,
    last_r,
    load_sem,
    mask_sem,
    in_sem,
    out_sem,
    tile_sem,
    gather_sem,
    sum_sem,
    last_sem,
):
    zhs, zls, cs = dims
    n = ab.shape[2]
    width = loaded.shape[2]
    tile = tile_ref.shape[2]
    rows = ab.shape[0]
    groups = rows // 2
    peers = zls * cs
    ring = zhs * peers
    chunk = min(CHUNK, n)
    chunks = n // chunk
    span = n // 8
    zh, zl, core = lax.axis_index("zh"), lax.axis_index("zl"), lax.axis_index("core")
    place = {"x": lax.axis_index("x"), "y": lax.axis_index("y")}
    me = zl * cs + core
    spot = zh * peers + me

    def remote(src, dst, sem, device):
        return pltpu.make_async_remote_copy(
            src_ref=src,
            dst_ref=dst,
            send_sem=sem.at[0],
            recv_sem=sem.at[1],
            device_id=device,
            device_id_type=MESH,
        )

    def peer_of(offset):
        other = lax.rem(me + offset, peers)
        return other, other // cs, lax.rem(other, cs)

    def ring_of(offset):
        other = lax.rem(spot + offset, ring)
        return other // peers, lax.rem(other, peers) // cs, lax.rem(other, cs)

    def ring_target(offset):
        h, z, c = ring_of(offset)
        return {"zh": h, "zl": z, "core": c}

    def step(axis, by):
        return lax.rem(place[axis] + by, 4)

    low_half = lax.broadcasted_iota(jnp.int32, (1, 1, LANES), 2) < LANES // 2

    def join(a, b):
        a, b = a.astype(F32), b.astype(F32)
        shape = a.shape
        turn = lambda v: pltpu.roll(v.reshape(-1, LANES), LANES // 2, 1).reshape(shape)
        return jnp.where(low_half, a, turn(b)).astype(BF16), jnp.where(low_half, turn(a), b).astype(BF16)

    def pack(group):
        def pack_chip(z, carry):
            at = pl.ds(z * rows + group * 2, 2)
            first = join(loaded[0, at], loaded[1, at])
            second = join(loaded[3, at], loaded[2, at])
            for c in range(2):
                send_ref[c, at, 0] = first[c]
                send_ref[c, at, 1] = second[c]
            return carry

        lax.fori_loop(0, zls, pack_chip, 0)

    def unpack(group):
        def unpack_chip(z, carry):
            at = z * rows + group * 2
            pair = zls * rows + z * groups + group
            value, key = join(out_ref[0, pl.ds(at, 2)], out_ref[1, pl.ds(at, 2)])
            dv_ref[pl.ds(at, 2)] = value
            dk_ref[pl.ds(at, 2)] = key
            even, odd = join(out_ref[0, pl.ds(pair, 1)], out_ref[1, pl.ds(pair, 1)])
            dq_ref[pl.ds(at, 1)] = even
            dq_ref[pl.ds(at + 1, 1)] = odd
            return carry

        lax.fori_loop(0, zls, unpack_chip, 0)

    barrier = pltpu.get_barrier_semaphore()
    for offset in range(1, ring):
        pl.semaphore_signal(barrier, inc=1, device_id=ring_target(offset), device_id_type=MESH)
    for axis in ("x", "y"):
        for by in (1, 3):
            pl.semaphore_signal(barrier, inc=1, device_id={axis: step(axis, by)}, device_id_type=MESH)
    loads = [
        pltpu.make_async_copy(ref, loaded.at[i], load_sem.at[i])
        for i, ref in enumerate((q_hbm, k_hbm, v_hbm, g_hbm))
    ]
    for load in loads:
        load.start()
    for z in range(zls):
        mask_ref[z] = 1000000000.0 * (mask_in[z * rows : (z + 1) * rows].astype(F32) - 1.0)
    for load in loads:
        load.wait()
    pack(0)
    pl.semaphore_wait(barrier, ring - 1 + 4)

    def columns_of(c):
        return pl.ds(pl.multiple_of(c * width, width), width)

    def tile_copy(offset):
        _, _, c = ring_of(offset)
        return remote(tile_ref.at[c], trecv.at[spot], tile_sem.at[offset], ring_target(offset))

    def mask_copy(offset):
        _, z, c = peer_of(offset)
        return remote(mask_ref.at[z], mrecv.at[me], mask_sem.at[offset], {"zl": z, "core": c})

    def in_copy(i, offset):
        _, z, c = peer_of(offset)
        return remote(
            send_ref.at[c, z * rows + i],
            ab.at[i, :, columns_of(me)],
            in_sem.at[i, offset],
            {"zl": z, "core": c},
        )

    def slot_of(i, pair):
        return (rows + i, zls * rows + zl * groups + i) if pair else (i, zl * rows + i)

    def out_copy(i, pair, offset):
        other, z, c = peer_of(offset)
        source, dest = slot_of(i, pair)
        return remote(
            obuf.at[source, columns_of(other)],
            out_ref.at[core, dest],
            out_sem.at[source, offset],
            {"zl": z, "core": c},
        )

    def out_start(i, pair):
        for offset in range(1, peers):
            out_copy(i, pair, offset).start()

    def out_keep(i, pair):
        source, dest = slot_of(i, pair)
        out_ref[core, dest] = obuf[source, columns_of(me)]

    orders = (("x", "y"), ("y", "x"))

    def block(h, phase, index, half):
        axis = orders[h][phase]
        other = "y" if axis == "x" else "x"
        at = {axis: index, other: place[other] if phase == 0 else slice(None)}
        return biasb.at[h, slice(None) if half is None else half, at["x"], at["y"]]

    def gather_copy(h, phase, hop, way):
        axis = orders[h][phase]
        by = (1, 3)[way]
        half = 1 - way if hop == 1 else way
        ref = block(h, phase, step(axis, 4 - by) if hop == 2 else place[axis], half)
        return remote(ref, ref, gather_sem.at[h, phase, hop, way], {axis: step(axis, by)})

    for offset in range(1, ring):
        tile_copy(offset).start()
    trecv[spot] = tile_ref[core]
    for offset in range(1, peers):
        mask_copy(offset).start()
    mrecv[me] = mask_ref[zl]
    for group in range(groups):
        if group:
            pack(group)
        for i in (group * 2, group * 2 + 1):
            for offset in range(1, peers):
                in_copy(i, offset).start()
        ab[group * 2 : group * 2 + 2, :, columns_of(me)] = send_ref[core, pl.ds(zl * rows + group * 2, 2)]

    gb[...] = jnp.zeros_like(gb)

    for offset in range(1, ring):
        tile_copy(offset).wait()
    for h in range(2):
        for z in range(zhs):
            pieces = [trecv[z * peers + c, h].astype(F32) for c in range(peers)]
            biasb[h, z, place["x"], place["y"]] = jnp.concatenate(pieces, axis=1).astype(BF16)
    for phase in range(2):
        for hop in range(2):
            for h in range(2):
                for way in range(2):
                    gather_copy(h, phase, hop, way).start()
        for h in range(2):
            for way in range(2):
                gather_copy(h, phase, 0, way).wait_recv()
                gather_copy(h, phase, 2, way).start()
        if phase == 0:
            for offset in range(1, peers):
                mask_copy(offset).wait()
            for s in range(peers):
                maskt[s * width : (s + 1) * width, :] = jnp.transpose(mrecv[s])
            for i in range(rows):
                maskf[i] = jnp.broadcast_to(maskt[:, i : i + 1], (n, LANES))
        for h in range(2):
            for way in range(2):
                gather_copy(h, phase, 0, way).wait_send()
                gather_copy(h, phase, 1, way).wait()
                gather_copy(h, phase, 2, way).wait()

    def widen(r, carry):
        for h in range(2):
            biasf[h, pl.ds(pl.multiple_of(r * tile, tile), tile), :] = biasb[
                h, r // 16, lax.rem(r // 4, 4), lax.rem(r, 4)
            ].astype(F32)
        return carry

    lax.fori_loop(0, n // tile, widen, 0)

    lane_head = lax.broadcasted_iota(jnp.int32, (1, LANES), 1) // HEAD_DIM

    def terms(h, a, zsel):
        axis = orders[h][0]
        return gb[h, zsel, a] if axis == "x" else gb[h, zsel, :, a]

    def first_copy(h, way):
        axis = orders[h][0]
        return remote(
            first_s.at[h, way], first_r.at[h, way], sum_sem.at[h, 0, way], {axis: step(axis, (1, 3)[way])}
        )

    def second_copy(h, way, z):
        axis = orders[h][0]
        return remote(
            second_s.at[h, way, z],
            second_r.at[h, way, z],
            sum_sem.at[h, 1 + z, way],
            {axis: step(axis, (1, 3)[way])},
        )

    def third_copy(h, way):
        axis = orders[h][1]
        return remote(
            third_s.at[h, way], third_r.at[h, way], sum_sem.at[h, 3, way], {axis: step(axis, (1, 3)[way])}
        )

    def fourth_copy(h, way, z):
        axis = orders[h][1]
        return remote(
            fourth_s.at[h, way, z],
            fourth_r.at[h, way, z],
            sum_sem.at[h, 4 + z, way],
            {axis: step(axis, (1, 3)[way])},
        )

    def sums_begin(h):
        axis = orders[h][0]
        for way in range(2):
            first_s[h, way] = terms(h, step(axis, 2), way).astype(BF16)
            first_copy(h, way).start()
        for way in range(2):
            second_s[h, way, 1 - way] = terms(h, step(axis, (1, 3)[way]), 1 - way).astype(BF16)
            second_copy(h, way, 1 - way).start()

    def sums_forward(h):
        axis = orders[h][0]
        for way in range(2):
            first_copy(h, way).wait()
            own = terms(h, step(axis, (1, 3)[way]), way)
            second_s[h, way, way] = (own + first_r[h, way].astype(F32)).astype(BF16)
            second_copy(h, way, way).start()

    def sums_turn(h):
        mine = place[orders[h][0]]
        axis = orders[h][1]
        for z in range(2):
            for way in range(2):
                second_copy(h, way, z).wait()
            partial[h, z] = terms(h, mine, z) + second_r[h, 0, z].astype(F32) + second_r[h, 1, z].astype(F32)
        for way in range(2):
            third_s[h, way] = partial[h, way, step(axis, 2)].astype(BF16)
            third_copy(h, way).start()
        for way in range(2):
            fourth_s[h, way, 1 - way] = partial[h, 1 - way, step(axis, (1, 3)[way])].astype(BF16)
            fourth_copy(h, way, 1 - way).start()

    def sums_close(h):
        axis = orders[h][1]
        for way in range(2):
            third_copy(h, way).wait()
            own = partial[h, way, step(axis, (1, 3)[way])]
            fourth_s[h, way, way] = (own + third_r[h, way].astype(F32)).astype(BF16)
            fourth_copy(h, way, way).start()

    def sums_last(h):
        mine = place[orders[h][1]]
        for z in range(2):
            for way in range(2):
                fourth_copy(h, way, z).wait()
            total = partial[h, z, mine] + fourth_r[h, 0, z].astype(F32) + fourth_r[h, 1, z].astype(F32)
            for c in range(peers):
                last_s[z * peers + c, h] = total[:, c * width : (c + 1) * width].astype(BF16)

    def last_copy(offset):
        return remote(
            last_s.at[lax.rem(spot + offset, ring)], last_r.at[spot], last_sem.at[offset], ring_target(offset)
        )

    def release(count):
        def release_row(i, carry):
            out_start(i, False)
            return carry

        def release_pair(i, carry):
            out_start(i, True)
            return carry

        lax.fori_loop(0, count, release_row, 0)
        lax.fori_loop(0, groups - 1, release_pair, 0)

    def one_row(i, last):
        for offset in range(1, peers):
            in_copy(i, offset).wait()
        if not last:
            pl.when(i == rows - 2)(lambda: release(rows - 2))
        a = ab[i, 0].astype(F32)
        b = ab[i, 1].astype(F32)
        ar = pltpu.roll(a, 64, 1)
        br = pltpu.roll(b, 64, 1)
        for h in range(2):
            kq[h] = jnp.where(lane_head == h, ar, 0.0).astype(BF16)
            kq[2 + h] = jnp.where(lane_head == 2 + h, ar, 0.0).astype(BF16)
            vg[h] = jnp.where(lane_head == h, br, 0.0).astype(BF16)
            vg[2 + h] = jnp.where(lane_head == h, b, 0.0).astype(BF16)
        kt[...] = jnp.transpose(ar).astype(BF16)
        vk[...] = jnp.zeros_like(vk)

        def columns(u):
            return pl.ds(pl.multiple_of(u * chunk, chunk), chunk)

        def scores(h, u):
            cols = columns(u)
            s = dot(kq[h], ab[i, 0, cols, :], ((1,), (1,)))
            top = None
            for k0 in range(0, n, span):
                m128 = maskf[i, k0 : k0 + span, :]
                mask = jnp.concatenate([m128] * (chunk // LANES), axis=1) if chunk > LANES else m128[:, :chunk]
                part = (s[k0 : k0 + span] * SCALE + biasf[h, k0 : k0 + span, cols]) + mask
                sbuf[h, k0 : k0 + span] = part
                part = jnp.max(part.reshape(-1, 8, chunk), axis=0)
                top = part if top is None else jnp.maximum(top, part)
            maxbuf[h] = top
            dpbuf[h] = dot(vg[h], ab[i, 1, cols, :], ((1,), (1,)))

        def soft(h, u):
            cols = columns(u)
            top = jnp.max(maxbuf[h], axis=0, keepdims=True)
            total = weighted = None
            for k0 in range(0, n, span):
                e = jnp.exp(sbuf[h, k0 : k0 + span] - top)
                sbuf[h, k0 : k0 + span] = e
                first = jnp.sum(e.reshape(-1, 8, chunk), axis=0)
                second = jnp.sum((e * dpbuf[h, k0 : k0 + span]).reshape(-1, 8, chunk), axis=0)
                total = first if total is None else total + first
                weighted = second if weighted is None else weighted + second
            inverse = 1.0 / jnp.sum(total, axis=0, keepdims=True)
            delta = jnp.sum(weighted, axis=0, keepdims=True) * inverse
            for b in range(8):
                k0 = b * span
                p = sbuf[h, k0 : k0 + span] * inverse
                ds = p * (dpbuf[h, k0 : k0 + span] - delta)
                pbuf[h, k0 : k0 + span] = p.astype(BF16)
                lowbuf[h, k0 : k0 + span] = ds.astype(BF16)
                gb[h, b // 4, b % 4, :, :, cols] += ds.reshape(4, tile, chunk)

        def grads(h, u):
            cols = columns(u)
            vk[...] += dot(pbuf[h], vg[2 + h, cols, :], ((1,), (0,))) + dot(
                lowbuf[h], kq[2 + h, cols, :], ((1,), (0,))
            )
            head_rows = kt[h * HEAD_DIM : (h + 1) * HEAD_DIM, :]
            at = pl.multiple_of(lax.rem(i, 2) * 64 + h * HEAD_DIM, HEAD_DIM)
            dqt[pl.ds(at, HEAD_DIM), cols] = dot(head_rows, lowbuf[h], ((1,), (0,)))

        pbuf[1] = jnp.zeros_like(pbuf[1])
        lowbuf[1] = jnp.zeros_like(lowbuf[1])
        scores(0, 0)

        def one_step(u, carry):
            scores(1, u)
            grads(1, lax.rem(u + chunks - 1, chunks))
            soft(0, u)
            scores(0, lax.rem(u + 1, chunks))
            grads(0, u)
            soft(1, u)
            return carry

        lax.fori_loop(0, chunks, one_step, 0)
        if last:
            sums_begin(0)
            sums_begin(1)
        grads(1, chunks - 1)
        obuf[i] = (vk[...] * jnp.where(lane_head < 2, 1.0, SCALE)).astype(BF16)
        if last:
            out_start(i, False)
        else:
            pl.when(i == rows - 2)(lambda: out_start(i, False))
        out_keep(i, False)

    def close_pair(pair):
        obuf[rows + pair] = (jnp.transpose(dqt[...]) * SCALE).astype(BF16)
        out_keep(pair, True)

    def early_row(i, carry):
        one_row(i, False)

        @pl.when(lax.rem(i, 2) == 1)
        def _():
            close_pair(i // 2)

        return carry

    lax.fori_loop(0, rows - 1, early_row, 0)
    one_row(rows - 1, True)
    sums_forward(0)
    sums_forward(1)
    close_pair(groups - 1)
    for stage in (sums_turn, sums_close, sums_last):
        for h in range(2):
            stage(h)
    for offset in range(1, ring):
        last_copy(offset).start()
    out_start(groups - 1, True)
    last_r[spot] = last_s[spot]

    def drain(group, carry):
        for offset in range(1, peers):
            out_copy(group * 2, False, offset).wait()
            out_copy(group * 2 + 1, False, offset).wait()
            out_copy(group, True, offset).wait()
        unpack(group)
        return carry

    lax.fori_loop(0, groups - 1, drain, 0)
    for offset in range(1, ring):
        last_copy(offset).wait()
    for c in range(cs):
        for h in range(2):
            total = last_r[c, h].astype(F32)
            for s in range(c + cs, ring, cs):
                total += last_r[s, h].astype(F32)
            gout_ref[2 * c + h] = total
    drain(groups - 1, 0)


def attention(dims, queries, keys, values, grads, mask, tiles):
    zhs, zls, cs = dims
    width = queries.shape[1]
    n = zls * cs * width
    rows = queries.shape[0] // zls
    chunk = min(CHUNK, n)
    groups = rows // 2
    peers = zls * cs
    ring = zhs * peers
    tile = tiles.shape[2]
    vmem_spec = pl.BlockSpec(memory_space=pltpu.VMEM)
    dma = pltpu.SemaphoreType.DMA
    return pl.pallas_call(
        functools.partial(kernel, dims),
        out_shape=(
            jax.ShapeDtypeStruct(queries.shape, BF16),
            jax.ShapeDtypeStruct(queries.shape, BF16),
            jax.ShapeDtypeStruct(queries.shape, BF16),
            jax.ShapeDtypeStruct((HEADS, tile, width), F32),
        ),
        in_specs=[pl.BlockSpec(memory_space=pl.ANY)] * 4 + [vmem_spec] * 2,
        out_specs=(vmem_spec,) * 4,
        scratch_shapes=[
            pltpu.VMEM((4, zls * rows, width, LANES), BF16),
            pltpu.VMEM((zls, rows, width), F32),
            pltpu.VMEM((cs, zls * rows, 2, width, LANES), BF16),
            pltpu.VMEM((cs, zls * (rows + groups), width, LANES), BF16),
            pltpu.VMEM((2, n, chunk), BF16),
            pltpu.VMEM((2, n, chunk), F32),
            pltpu.VMEM((2, n, chunk), F32),
            pltpu.VMEM((2, n, chunk), BF16),
            pltpu.VMEM((2, 8, chunk), F32),
            pltpu.VMEM((rows, 2, n, LANES), BF16),
            pltpu.VMEM((2, 2, 4, 4, tile, n), BF16),
            pltpu.VMEM((2, n, n), F32),
            pltpu.VMEM((2, 2, 4, 4, tile, n), F32),
            pltpu.VMEM((peers, rows, width), F32),
            pltpu.VMEM((n, rows), F32),
            pltpu.VMEM((rows, n, LANES), F32),
            pltpu.VMEM((4, n, LANES), BF16),
            pltpu.VMEM((4, n, LANES), BF16),
            pltpu.VMEM((LANES, n), BF16),
            pltpu.VMEM((n, LANES), F32),
            pltpu.VMEM((LANES, n), F32),
            pltpu.VMEM((rows + groups, n, LANES), BF16),
            pltpu.VMEM((ring, 2, tile, width), BF16),
            pltpu.VMEM((2, 2, 4, tile, n), BF16),
            pltpu.VMEM((2, 2, 4, tile, n), BF16),
            pltpu.VMEM((2, 2, 2, 4, tile, n), BF16),
            pltpu.VMEM((2, 2, 2, 4, tile, n), BF16),
            pltpu.VMEM((2, 2, 4, tile, n), F32),
            pltpu.VMEM((2, 2, tile, n), BF16),
            pltpu.VMEM((2, 2, tile, n), BF16),
            pltpu.VMEM((2, 2, 2, tile, n), BF16),
            pltpu.VMEM((2, 2, 2, tile, n), BF16),
            pltpu.VMEM((ring, 2, tile, width), BF16),
            pltpu.VMEM((ring, 2, tile, width), BF16),
            dma((4,)),
            dma((peers, 2)),
            dma((rows, peers, 2)),
            dma((rows + groups, peers, 2)),
            dma((ring, 2)),
            dma((2, 2, 3, 2, 2)),
            dma((2, 6, 2, 2)),
            dma((ring, 2)),
        ],
        compiler_params=pltpu.CompilerParams(
            collective_id=0, has_side_effects=True, vmem_limit_bytes=52 * 1024 * 1024
        ),
        cost_estimate=pl.CostEstimate(
            flops=10 * rows * 2 * n * n * LANES, bytes_accessed=32 * 1024 * 1024, transcendentals=0
        ),
        name="attention_backward",
    )(queries, keys, values, grads, mask, tiles)


def settle_kernel(*refs):
    count = len(refs) // 2
    sem = refs[-1]
    copies = [pltpu.make_async_copy(refs[i], refs[count + i], sem.at[i]) for i in range(count)]
    for copy in copies:
        copy.start()
    for copy in copies:
        copy.wait()


def settle(*arrays):
    count = len(arrays)
    return pl.pallas_call(
        settle_kernel,
        out_shape=tuple(jax.ShapeDtypeStruct(a.shape, a.dtype) for a in arrays),
        in_specs=[pl.BlockSpec(memory_space=pltpu.VMEM)] * count,
        out_specs=(pl.BlockSpec(memory_space=pl.ANY),) * count,
        scratch_shapes=[pltpu.SemaphoreType.DMA((count,))],
        compiler_params=pltpu.CompilerParams(vmem_limit_bytes=8 * 1024 * 1024),
        name="settle",
    )(*arrays)


def local(zhs, zs, cs, query_proj, key_proj, value_proj, pair_bias, pair_mask, grad_out):
    width = query_proj.shape[1]
    tile = pair_bias.shape[2]
    tiles = jnp.transpose(pair_bias, (0, 2, 1)).reshape(cs, 2, tile, width)
    grad_query, grad_key, grad_value, gb = attention(
        (zhs, zs, cs), query_proj, key_proj, value_proj, grad_out, pair_mask, tiles
    )
    grad_query, grad_key, grad_value, gb = settle(grad_query, grad_key, grad_value, gb)
    return grad_query, grad_key, grad_value, jnp.transpose(gb, (0, 2, 1))


def solution(mesh):
    shape = (2, 4, 4, mesh.shape["col"] // 2, 2)
    torus = Mesh(mesh.devices.reshape(shape), ROW + COL)
    pair = P(ROW, COL, None)
    tile = P(None, COL, ROW)
    return jax.shard_map(
        functools.partial(local, shape[0], shape[3], shape[4]),
        mesh=torus,
        in_specs=(pair, pair, pair, tile, P(ROW, COL), pair),
        out_specs=(pair, pair, pair, tile),
        check_vma=False,
    )
```

```python
import functools
import math

import jax
import jax.numpy as jnp
from jax import lax
from jax.experimental import pallas as pl
from jax.experimental.pallas import tpu as pltpu
from jax.sharding import Mesh
from jax.sharding import PartitionSpec as P

HEADS = 4
HEAD_DIM = 32
SCALE = 1.0 / math.sqrt(HEAD_DIM)
ROW = ("zh", "x", "y")
COL = ("zl", "core")
MESH = pl.DeviceIdType.MESH
LANES = 128
CHUNK = 256
F32 = jnp.float32
BF16 = jnp.bfloat16


def dot(a, b, dims):
    return lax.dot_general(a, b, (dims, ((), ())), preferred_element_type=F32)


def kernel(
    dims,
    q_hbm,
    k_hbm,
    v_hbm,
    g_hbm,
    mask_in,
    tile_ref,
    dq_ref,
    dk_ref,
    dv_ref,
    gout_ref,
    loaded,
    mask_ref,
    send_ref,
    out_ref,
    pbuf,
    sbuf,
    dpbuf,
    lowbuf,
    maxbuf,
    ab,
    biasb,
    biasf,
    gb,
    mrecv,
    maskt,
    maskf,
    kq,
    vg,
    kt,
    vk,
    dqt,
    obuf,
    trecv,
    first_s,
    first_r,
    second_s,
    second_r,
    partial,
    third_s,
    third_r,
    fourth_s,
    fourth_r,
    last_s,
    last_r,
    load_sem,
    mask_sem,
    in_sem,
    out_sem,
    tile_sem,
    gather_sem,
    sum_sem,
    last_sem,
):
    zhs, zls, cs = dims
    n = ab.shape[2]
    width = loaded.shape[2]
    tile = tile_ref.shape[2]
    rows = ab.shape[0]
    groups = rows // 2
    peers = zls * cs
    ring = zhs * peers
    chunk = min(CHUNK, n)
    chunks = n // chunk
    span = n // 8
    zh, zl, core = lax.axis_index("zh"), lax.axis_index("zl"), lax.axis_index("core")
    place = {"x": lax.axis_index("x"), "y": lax.axis_index("y")}
    me = zl * cs + core
    spot = zh * peers + me

    def remote(src, dst, sem, device):
        return pltpu.make_async_remote_copy(
            src_ref=src,
            dst_ref=dst,
            send_sem=sem.at[0],
            recv_sem=sem.at[1],
            device_id=device,
            device_id_type=MESH,
        )

    def peer_of(offset):
        other = lax.rem(me + offset, peers)
        return other, other // cs, lax.rem(other, cs)

    def ring_of(offset):
        other = lax.rem(spot + offset, ring)
        return other // peers, lax.rem(other, peers) // cs, lax.rem(other, cs)

    def ring_target(offset):
        h, z, c = ring_of(offset)
        return {"zh": h, "zl": z, "core": c}

    def step(axis, by):
        return lax.rem(place[axis] + by, 4)

    low_half = lax.broadcasted_iota(jnp.int32, (1, 1, LANES), 2) < LANES // 2

    def join(a, b):
        a, b = a.astype(F32), b.astype(F32)
        shape = a.shape
        turn = lambda v: pltpu.roll(v.reshape(-1, LANES), LANES // 2, 1).reshape(shape)
        return jnp.where(low_half, a, turn(b)).astype(BF16), jnp.where(low_half, turn(a), b).astype(BF16)

    def pack(group):
        def pack_chip(z, carry):
            at = pl.ds(z * rows + group * 2, 2)
            first = join(loaded[0, at], loaded[1, at])
            second = join(loaded[3, at], loaded[2, at])
            for c in range(2):
                send_ref[c, at, 0] = first[c]
                send_ref[c, at, 1] = second[c]
            return carry

        lax.fori_loop(0, zls, pack_chip, 0)

    def unpack(group):
        def unpack_chip(z, carry):
            at = z * rows + group * 2
            pair = zls * rows + z * groups + group
            value, key = join(out_ref[0, pl.ds(at, 2)], out_ref[1, pl.ds(at, 2)])
            dv_ref[pl.ds(at, 2)] = value
            dk_ref[pl.ds(at, 2)] = key
            even, odd = join(out_ref[0, pl.ds(pair, 1)], out_ref[1, pl.ds(pair, 1)])
            dq_ref[pl.ds(at, 1)] = even
            dq_ref[pl.ds(at + 1, 1)] = odd
            return carry

        lax.fori_loop(0, zls, unpack_chip, 0)

    barrier = pltpu.get_barrier_semaphore()
    for offset in range(1, ring):
        pl.semaphore_signal(barrier, inc=1, device_id=ring_target(offset), device_id_type=MESH)
    for axis in ("x", "y"):
        for by in (1, 3):
            pl.semaphore_signal(barrier, inc=1, device_id={axis: step(axis, by)}, device_id_type=MESH)
    loads = [
        pltpu.make_async_copy(ref, loaded.at[i], load_sem.at[i])
        for i, ref in enumerate((q_hbm, k_hbm, v_hbm, g_hbm))
    ]
    for load in loads:
        load.start()
    for z in range(zls):
        mask_ref[z] = 1000000000.0 * (mask_in[z * rows : (z + 1) * rows].astype(F32) - 1.0)
    for load in loads:
        load.wait()
    pack(0)
    pl.semaphore_wait(barrier, ring - 1 + 4)

    def columns_of(c):
        return pl.ds(pl.multiple_of(c * width, width), width)

    def tile_copy(offset):
        _, _, c = ring_of(offset)
        return remote(tile_ref.at[c], trecv.at[spot], tile_sem.at[offset], ring_target(offset))

    def mask_copy(offset):
        _, z, c = peer_of(offset)
        return remote(mask_ref.at[z], mrecv.at[me], mask_sem.at[offset], {"zl": z, "core": c})

    def in_copy(i, offset):
        _, z, c = peer_of(offset)
        return remote(
            send_ref.at[c, z * rows + i],
            ab.at[i, :, columns_of(me)],
            in_sem.at[i, offset],
            {"zl": z, "core": c},
        )

    def slot_of(i, pair):
        return (rows + i, zls * rows + zl * groups + i) if pair else (i, zl * rows + i)

    def out_copy(i, pair, offset):
        other, z, c = peer_of(offset)
        source, dest = slot_of(i, pair)
        return remote(
            obuf.at[source, columns_of(other)],
            out_ref.at[core, dest],
            out_sem.at[source, offset],
            {"zl": z, "core": c},
        )

    def out_start(i, pair):
        for offset in range(1, peers):
            out_copy(i, pair, offset).start()

    def out_keep(i, pair):
        source, dest = slot_of(i, pair)
        out_ref[core, dest] = obuf[source, columns_of(me)]

    orders = (("x", "y"), ("y", "x"))

    def block(h, phase, index, half):
        axis = orders[h][phase]
        other = "y" if axis == "x" else "x"
        at = {axis: index, other: place[other] if phase == 0 else slice(None)}
        return biasb.at[h, slice(None) if half is None else half, at["x"], at["y"]]

    def gather_copy(h, phase, hop, way):
        axis = orders[h][phase]
        by = (1, 3)[way]
        half = 1 - way if hop == 1 else way
        ref = block(h, phase, step(axis, 4 - by) if hop == 2 else place[axis], half)
        return remote(ref, ref, gather_sem.at[h, phase, hop, way], {axis: step(axis, by)})

    for offset in range(1, ring):
        tile_copy(offset).start()
    trecv[spot] = tile_ref[core]
    for offset in range(1, peers):
        mask_copy(offset).start()
    mrecv[me] = mask_ref[zl]
    for group in range(groups):
        if group:
            pack(group)
        for i in (group * 2, group * 2 + 1):
            for offset in range(1, peers):
                in_copy(i, offset).start()
        ab[group * 2 : group * 2 + 2, :, columns_of(me)] = send_ref[core, pl.ds(zl * rows + group * 2, 2)]

    gb[...] = jnp.zeros_like(gb)

    for offset in range(1, ring):
        tile_copy(offset).wait()
    for h in range(2):
        for z in range(zhs):
            pieces = [trecv[z * peers + c, h].astype(F32) for c in range(peers)]
            biasb[h, z, place["x"], place["y"]] = jnp.concatenate(pieces, axis=1).astype(BF16)
    for phase in range(2):
        for hop in range(2):
            for h in range(2):
                for way in range(2):
                    gather_copy(h, phase, hop, way).start()
        for h in range(2):
            for way in range(2):
                gather_copy(h, phase, 0, way).wait_recv()
                gather_copy(h, phase, 2, way).start()
        if phase == 0:
            for offset in range(1, peers):
                mask_copy(offset).wait()
            for s in range(peers):
                maskt[s * width : (s + 1) * width, :] = jnp.transpose(mrecv[s])
            for i in range(rows):
                maskf[i] = jnp.broadcast_to(maskt[:, i : i + 1], (n, LANES))
        for h in range(2):
            for way in range(2):
                gather_copy(h, phase, 0, way).wait_send()
                gather_copy(h, phase, 1, way).wait()
                gather_copy(h, phase, 2, way).wait()

    def widen(r, carry):
        for h in range(2):
            biasf[h, pl.ds(pl.multiple_of(r * tile, tile), tile), :] = biasb[
                h, r // 16, lax.rem(r // 4, 4), lax.rem(r, 4)
            ].astype(F32)
        return carry

    lax.fori_loop(0, n // tile, widen, 0)

    lane_head = lax.broadcasted_iota(jnp.int32, (1, LANES), 1) // HEAD_DIM

    def terms(h, a, zsel):
        axis = orders[h][0]
        return gb[h, zsel, a] if axis == "x" else gb[h, zsel, :, a]

    def first_copy(h, way):
        axis = orders[h][0]
        return remote(
            first_s.at[h, way], first_r.at[h, way], sum_sem.at[h, 0, way], {axis: step(axis, (1, 3)[way])}
        )

    def second_copy(h, way, z):
        axis = orders[h][0]
        return remote(
            second_s.at[h, way, z],
            second_r.at[h, way, z],
            sum_sem.at[h, 1 + z, way],
            {axis: step(axis, (1, 3)[way])},
        )

    def third_copy(h, way):
        axis = orders[h][1]
        return remote(
            third_s.at[h, way], third_r.at[h, way], sum_sem.at[h, 3, way], {axis: step(axis, (1, 3)[way])}
        )

    def fourth_copy(h, way, z):
        axis = orders[h][1]
        return remote(
            fourth_s.at[h, way, z],
            fourth_r.at[h, way, z],
            sum_sem.at[h, 4 + z, way],
            {axis: step(axis, (1, 3)[way])},
        )

    def sums_begin(h):
        axis = orders[h][0]
        for way in range(2):
            first_s[h, way] = terms(h, step(axis, 2), way).astype(BF16)
            first_copy(h, way).start()

    def sums_early(h):
        axis = orders[h][0]
        for way in range(2):
            second_s[h, way, 1 - way] = terms(h, step(axis, (1, 3)[way]), 1 - way).astype(BF16)
            second_copy(h, way, 1 - way).start()

    def sums_forward(h):
        axis = orders[h][0]
        for way in range(2):
            first_copy(h, way).wait()
            own = terms(h, step(axis, (1, 3)[way]), way)
            second_s[h, way, way] = (own + first_r[h, way].astype(F32)).astype(BF16)
            second_copy(h, way, way).start()

    def sums_turn(h):
        mine = place[orders[h][0]]
        axis = orders[h][1]
        for z in range(2):
            for way in range(2):
                second_copy(h, way, z).wait()
            partial[h, z] = terms(h, mine, z) + second_r[h, 0, z].astype(F32) + second_r[h, 1, z].astype(F32)
        for way in range(2):
            third_s[h, way] = partial[h, way, step(axis, 2)].astype(BF16)
            third_copy(h, way).start()
        for way in range(2):
            fourth_s[h, way, 1 - way] = partial[h, 1 - way, step(axis, (1, 3)[way])].astype(BF16)
            fourth_copy(h, way, 1 - way).start()

    def sums_close(h):
        axis = orders[h][1]
        for way in range(2):
            third_copy(h, way).wait()
            own = partial[h, way, step(axis, (1, 3)[way])]
            fourth_s[h, way, way] = (own + third_r[h, way].astype(F32)).astype(BF16)
            fourth_copy(h, way, way).start()

    def sums_last(h):
        mine = place[orders[h][1]]
        for z in range(2):
            for way in range(2):
                fourth_copy(h, way, z).wait()
            total = partial[h, z, mine] + fourth_r[h, 0, z].astype(F32) + fourth_r[h, 1, z].astype(F32)
            for c in range(peers):
                last_s[z * peers + c, h] = total[:, c * width : (c + 1) * width].astype(BF16)

    def last_copy(offset):
        return remote(
            last_s.at[lax.rem(spot + offset, ring)], last_r.at[spot], last_sem.at[offset], ring_target(offset)
        )

    def release(count):
        def release_row(i, carry):
            out_start(i, False)
            return carry

        def release_pair(i, carry):
            out_start(i, True)
            return carry

        lax.fori_loop(0, count, release_row, 0)
        lax.fori_loop(0, groups - 1, release_pair, 0)

    def one_row(i, last):
        for offset in range(1, peers):
            in_copy(i, offset).wait()
        if not last:
            pl.when(i == rows - 2)(lambda: release(rows - 2))
        a = ab[i, 0].astype(F32)
        b = ab[i, 1].astype(F32)
        ar = pltpu.roll(a, 64, 1)
        br = pltpu.roll(b, 64, 1)
        for h in range(2):
            kq[h] = jnp.where(lane_head == h, ar, 0.0).astype(BF16)
            kq[2 + h] = jnp.where(lane_head == 2 + h, ar, 0.0).astype(BF16)
            vg[h] = jnp.where(lane_head == h, br, 0.0).astype(BF16)
            vg[2 + h] = jnp.where(lane_head == h, b, 0.0).astype(BF16)
        kt[...] = jnp.transpose(ar).astype(BF16)
        vk[...] = jnp.zeros_like(vk)

        def columns(u):
            return pl.ds(pl.multiple_of(u * chunk, chunk), chunk)

        def scores(h, u):
            cols = columns(u)
            s = dot(kq[h], ab[i, 0, cols, :], ((1,), (1,)))
            top = None
            for k0 in range(0, n, span):
                m128 = maskf[i, k0 : k0 + span, :]
                mask = jnp.concatenate([m128] * (chunk // LANES), axis=1) if chunk > LANES else m128[:, :chunk]
                part = (s[k0 : k0 + span] * SCALE + biasf[h, k0 : k0 + span, cols]) + mask
                sbuf[h, k0 : k0 + span] = part
                part = jnp.max(part.reshape(-1, 8, chunk), axis=0)
                top = part if top is None else jnp.maximum(top, part)
            maxbuf[h] = top
            dpbuf[h] = dot(vg[h], ab[i, 1, cols, :], ((1,), (1,)))

        def soft(h, u):
            cols = columns(u)
            top = jnp.max(maxbuf[h], axis=0, keepdims=True)
            total = weighted = None
            for k0 in range(0, n, span):
                e = jnp.exp(sbuf[h, k0 : k0 + span] - top)
                sbuf[h, k0 : k0 + span] = e
                first = jnp.sum(e.reshape(-1, 8, chunk), axis=0)
                second = jnp.sum((e * dpbuf[h, k0 : k0 + span]).reshape(-1, 8, chunk), axis=0)
                total = first if total is None else total + first
                weighted = second if weighted is None else weighted + second
            inverse = 1.0 / jnp.sum(total, axis=0, keepdims=True)
            delta = jnp.sum(weighted, axis=0, keepdims=True) * inverse
            for b in range(8):
                k0 = b * span
                p = sbuf[h, k0 : k0 + span] * inverse
                ds = p * (dpbuf[h, k0 : k0 + span] - delta)
                pbuf[h, k0 : k0 + span] = p.astype(BF16)
                lowbuf[h, k0 : k0 + span] = ds.astype(BF16)
                gb[h, b // 4, b % 4, :, :, cols] += ds.reshape(4, tile, chunk)

        def grads(h, u):
            cols = columns(u)
            vk[...] += dot(pbuf[h], vg[2 + h, cols, :], ((1,), (0,))) + dot(
                lowbuf[h], kq[2 + h, cols, :], ((1,), (0,))
            )
            head_rows = kt[h * HEAD_DIM : (h + 1) * HEAD_DIM, :]
            at = pl.multiple_of(lax.rem(i, 2) * 64 + h * HEAD_DIM, HEAD_DIM)
            dqt[pl.ds(at, HEAD_DIM), cols] = dot(head_rows, lowbuf[h], ((1,), (0,)))

        pbuf[1] = jnp.zeros_like(pbuf[1])
        lowbuf[1] = jnp.zeros_like(lowbuf[1])
        scores(0, 0)

        def one_step(u, carry):
            scores(1, u)
            grads(1, lax.rem(u + chunks - 1, chunks))
            soft(0, u)
            scores(0, lax.rem(u + 1, chunks))
            grads(0, u)
            soft(1, u)
            return carry

        lax.fori_loop(0, chunks, one_step, 0)
        if last:
            sums_begin(0)
            sums_begin(1)
            sums_early(0)
            sums_early(1)
        grads(1, chunks - 1)
        obuf[i] = (vk[...] * jnp.where(lane_head < 2, 1.0, SCALE)).astype(BF16)
        if last:
            out_start(i, False)
        else:
            pl.when(i == rows - 2)(lambda: out_start(i, False))
        out_keep(i, False)

    def close_pair(pair):
        obuf[rows + pair] = (jnp.transpose(dqt[...]) * SCALE).astype(BF16)
        out_keep(pair, True)

    def early_row(i, carry):
        one_row(i, False)

        @pl.when(lax.rem(i, 2) == 1)
        def _():
            close_pair(i // 2)

        return carry

    lax.fori_loop(0, rows - 1, early_row, 0)
    one_row(rows - 1, True)
    sums_forward(0)
    sums_forward(1)
    close_pair(groups - 1)
    for stage in (sums_turn, sums_close, sums_last):
        for h in range(2):
            stage(h)
    for offset in range(1, ring):
        last_copy(offset).start()
    out_start(groups - 1, True)
    last_r[spot] = last_s[spot]

    def drain(group, carry):
        for offset in range(1, peers):
            out_copy(group * 2, False, offset).wait()
            out_copy(group * 2 + 1, False, offset).wait()
            out_copy(group, True, offset).wait()
        unpack(group)
        return carry

    lax.fori_loop(0, groups - 1, drain, 0)
    for offset in range(1, ring):
        last_copy(offset).wait()
    for c in range(cs):
        for h in range(2):
            total = last_r[c, h].astype(F32)
            for s in range(c + cs, ring, cs):
                total += last_r[s, h].astype(F32)
            gout_ref[2 * c + h] = total
    drain(groups - 1, 0)


def attention(dims, queries, keys, values, grads, mask, tiles):
    zhs, zls, cs = dims
    width = queries.shape[1]
    n = zls * cs * width
    rows = queries.shape[0] // zls
    chunk = min(CHUNK, n)
    groups = rows // 2
    peers = zls * cs
    ring = zhs * peers
    tile = tiles.shape[2]
    vmem_spec = pl.BlockSpec(memory_space=pltpu.VMEM)
    dma = pltpu.SemaphoreType.DMA
    return pl.pallas_call(
        functools.partial(kernel, dims),
        out_shape=(
            jax.ShapeDtypeStruct(queries.shape, BF16),
            jax.ShapeDtypeStruct(queries.shape, BF16),
            jax.ShapeDtypeStruct(queries.shape, BF16),
            jax.ShapeDtypeStruct((HEADS, tile, width), F32),
        ),
        in_specs=[pl.BlockSpec(memory_space=pl.ANY)] * 4 + [vmem_spec] * 2,
        out_specs=(vmem_spec,) * 4,
        scratch_shapes=[
            pltpu.VMEM((4, zls * rows, width, LANES), BF16),
            pltpu.VMEM((zls, rows, width), F32),
            pltpu.VMEM((cs, zls * rows, 2, width, LANES), BF16),
            pltpu.VMEM((cs, zls * (rows + groups), width, LANES), BF16),
            pltpu.VMEM((2, n, chunk), BF16),
            pltpu.VMEM((2, n, chunk), F32),
            pltpu.VMEM((2, n, chunk), F32),
            pltpu.VMEM((2, n, chunk), BF16),
            pltpu.VMEM((2, 8, chunk), F32),
            pltpu.VMEM((rows, 2, n, LANES), BF16),
            pltpu.VMEM((2, 2, 4, 4, tile, n), BF16),
            pltpu.VMEM((2, n, n), F32),
            pltpu.VMEM((2, 2, 4, 4, tile, n), F32),
            pltpu.VMEM((peers, rows, width), F32),
            pltpu.VMEM((n, rows), F32),
            pltpu.VMEM((rows, n, LANES), F32),
            pltpu.VMEM((4, n, LANES), BF16),
            pltpu.VMEM((4, n, LANES), BF16),
            pltpu.VMEM((LANES, n), BF16),
            pltpu.VMEM((n, LANES), F32),
            pltpu.VMEM((LANES, n), F32),
            pltpu.VMEM((rows + groups, n, LANES), BF16),
            pltpu.VMEM((ring, 2, tile, width), BF16),
            pltpu.VMEM((2, 2, 4, tile, n), BF16),
            pltpu.VMEM((2, 2, 4, tile, n), BF16),
            pltpu.VMEM((2, 2, 2, 4, tile, n), BF16),
            pltpu.VMEM((2, 2, 2, 4, tile, n), BF16),
            pltpu.VMEM((2, 2, 4, tile, n), F32),
            pltpu.VMEM((2, 2, tile, n), BF16),
            pltpu.VMEM((2, 2, tile, n), BF16),
            pltpu.VMEM((2, 2, 2, tile, n), BF16),
            pltpu.VMEM((2, 2, 2, tile, n), BF16),
            pltpu.VMEM((ring, 2, tile, width), BF16),
            pltpu.VMEM((ring, 2, tile, width), BF16),
            dma((4,)),
            dma((peers, 2)),
            dma((rows, peers, 2)),
            dma((rows + groups, peers, 2)),
            dma((ring, 2)),
            dma((2, 2, 3, 2, 2)),
            dma((2, 6, 2, 2)),
            dma((ring, 2)),
        ],
        compiler_params=pltpu.CompilerParams(
            collective_id=0, has_side_effects=True, vmem_limit_bytes=52 * 1024 * 1024
        ),
        cost_estimate=pl.CostEstimate(
            flops=10 * rows * 2 * n * n * LANES, bytes_accessed=32 * 1024 * 1024, transcendentals=0
        ),
        name="attention_backward",
    )(queries, keys, values, grads, mask, tiles)


def settle_kernel(*refs):
    count = len(refs) // 2
    sem = refs[-1]
    copies = [pltpu.make_async_copy(refs[i], refs[count + i], sem.at[i]) for i in range(count)]
    for copy in copies:
        copy.start()
    for copy in copies:
        copy.wait()


def settle(*arrays):
    count = len(arrays)
    return pl.pallas_call(
        settle_kernel,
        out_shape=tuple(jax.ShapeDtypeStruct(a.shape, a.dtype) for a in arrays),
        in_specs=[pl.BlockSpec(memory_space=pltpu.VMEM)] * count,
        out_specs=(pl.BlockSpec(memory_space=pl.ANY),) * count,
        scratch_shapes=[pltpu.SemaphoreType.DMA((count,))],
        compiler_params=pltpu.CompilerParams(vmem_limit_bytes=8 * 1024 * 1024),
        name="settle",
    )(*arrays)


def local(zhs, zs, cs, query_proj, key_proj, value_proj, pair_bias, pair_mask, grad_out):
    width = query_proj.shape[1]
    tile = pair_bias.shape[2]
    tiles = jnp.transpose(pair_bias, (0, 2, 1)).reshape(cs, 2, tile, width)
    grad_query, grad_key, grad_value, gb = attention(
        (zhs, zs, cs), query_proj, key_proj, value_proj, grad_out, pair_mask, tiles
    )
    grad_query, grad_key, grad_value, gb = settle(grad_query, grad_key, grad_value, gb)
    return grad_query, grad_key, grad_value, jnp.transpose(gb, (0, 2, 1))


def solution(mesh):
    shape = (2, 4, 4, mesh.shape["col"] // 2, 2)
    torus = Mesh(mesh.devices.reshape(shape), ROW + COL)
    pair = P(ROW, COL, None)
    tile = P(None, COL, ROW)
    return jax.shard_map(
        functools.partial(local, shape[0], shape[3], shape[4]),
        mesh=torus,
        in_specs=(pair, pair, pair, tile, P(ROW, COL), pair),
        out_specs=(pair, pair, pair, tile),
        check_vma=False,
    )
```
